256 devices in a mesh: planes: 64 (over y, z_hi, x, core), elem: 4 (over z_lo).
Axes of the slice: x: 4, y: 4, z: 8 (z_hi: 2, z_lo: 4; z = z_hi * 4 + z_lo), core: 2. Of those that a mesh axis runs over, the one named last changes fastest.
Arguments:
- velocity: float32 [3, 256, 41472], P(None, 'planes', 'elem'), may hold values from -6 to 6
- geometry: float32 [4, 41472], P(None, 'elem'), may hold values from -1.5 to 1.5
- element_kind: int32 [512], P('elem'), may hold values from 0 to 1
- element_scale: float32 [512], P('elem'), may hold values from 0.5 to 2
- dirichlet: int32 [2, 9, 512], P(None, None, 'elem'), may hold values 0 or 1
- schur_stiffness: float32 [2, 36, 36], replicated, may hold values from -0.2 to 8.5, as said below
- schur_mass: float32 [2, 36, 36], replicated, may hold values from -0.1 to 4.5, as said below
- lift: float32 [2, 36, 81], replicated, may hold values from -0.625 to 0.625
- recover: float32 [2, 81, 36], replicated, may hold values from -1 to 1
Outputs:
- new_velocity: float32 [3, 256, 41472], P(None, 'planes', 'elem')
The draws below stay inside these ranges and needn't reach their ends.
Inputs may be any that keep to these rules, and one draw needn't show every extreme that they name: `schur_stiffness`: each of the two matrices is symmetric and positive definite. `schur_mass`: each of the two matrices is symmetric and positive definite.
All inputs are finite; a program needn't handle non-finite values. No bound on the sum of `dirichlet` on one device may be relied on, other than what follows from the above.
Results may differ from the reference program's by a relative error of at most 0.0001.
Values sent between devices are 32-bit elements; how exact they have to be, the bound alone decides.
No kernel may reach another device: no remote copies, remote signals or barrier semaphores. Data moves between devices by JAX's collectives and lax.ppermute only.
A program may use at most 128 MiB of HBM per device.

```python
import math
import jax
import jax.numpy as jnp
import numpy as np
from jax import lax

PLANES = 256
QUAD = 9
COLUMN_ELEMS = 32
CG_STEPS = 4
ELEMS = 512
NODES = 41472


def symmetric_dominant(key, off_scale, lo, hi):
    size = 4 * QUAD
    keys = jax.random.split(key, 2)
    upper = jnp.triu(jax.random.uniform(keys[0], (2, size, size), jnp.float32, -off_scale, off_scale), 1)
    off_part = upper + jnp.swapaxes(upper, 1, 2)
    rowsum = jnp.sum(jnp.abs(off_part), axis=2)
    extra = jax.random.uniform(keys[1], (2, size), jnp.float32, lo, hi)
    return off_part + jnp.eye(size, dtype=jnp.float32)[None] * (rowsum + extra)[:, :, None]


def draw_schur_stiffness(key, part):
    return symmetric_dominant(jax.random.fold_in(key, 11), 0.2, 0.5, 1.5)


def draw_schur_mass(key, part):
    return symmetric_dominant(jax.random.fold_in(key, 23), 0.1, 0.5, 1.0)


def place_ends(result, stream_key, low, largest):
    index_at = [jax.random.randint(jax.random.fold_in(stream_key, axis), (), 0, length) for axis, length in enumerate(result.shape)]
    longest = result.shape.index(max(result.shape))
    neighbour = index_at[:longest] + [(index_at[longest] + 1) % result.shape[longest]] + index_at[longest + 1:]
    return result.at[tuple(index_at)].set(low).at[tuple(neighbour)].set(largest)


def block_levels(key, dims, cuts, least, largest):
    def one(position, blocks):
        steps = jax.random.uniform(jax.random.fold_in(jax.random.fold_in(key, 6), position), (blocks,), jnp.float32, least / len(cuts), largest / len(cuts))
        return jnp.repeat(jnp.exp(steps), dims[position] // blocks).reshape((-1,) + (1,) * (len(dims) - position - 1))

    gain = one(*cuts[0])
    for cut in cuts[1:]:
        gain = gain * one(*cut)
    return gain


def centred(stream_key, extent, deviation, bound, shards=(), kind=jnp.bfloat16):
    factor_of = block_levels(stream_key, extent, shards, -0.22, 0.18) if shards else 1.0
    result = jax.random.normal(stream_key, extent, jnp.float32) * deviation * factor_of
    return jnp.minimum(jnp.maximum(result, -bound), bound).astype(kind)


def setup_inputs(seed: int = 0) -> dict:
    streams_of = jax.random.split(jax.random.key(seed), 10)
    velocity = centred(streams_of[0], (3, PLANES, NODES), 1.0, 6.0, ((1, 64), (2, 4)), jnp.float32)
    geometry = jnp.clip(jax.random.uniform(streams_of[1], (4, NODES), jnp.float32, -1.5, 1.5) * block_levels(streams_of[1], (4, NODES), ((1, 4),), -0.4, 0.0), -1.5, 1.5)
    element_kind = place_ends(jax.random.randint(streams_of[2], (ELEMS,), 0, 2), jax.random.fold_in(streams_of[2], 1), 0, 1).astype(jnp.int32)
    element_scale = jnp.clip(jnp.exp(math.log(2.0) - 1.3862944 * jax.random.uniform(streams_of[3], (ELEMS,), jnp.float32) ** block_levels(streams_of[3], (ELEMS,), ((0, 4),), -0.2, 0.2)), 0.5, 2.0)
    dirichlet = place_ends((jax.random.randint(streams_of[4], (2, QUAD, ELEMS), 0, 6) < 1).astype(jnp.int32), jax.random.fold_in(streams_of[4], 1), 0, 1)
    schur_stiffness = draw_schur_stiffness(jax.random.fold_in(streams_of[9], 71), 0)
    schur_mass = draw_schur_mass(jax.random.fold_in(streams_of[9], 71), 0)
    lift = centred(streams_of[7], (2, 4 * QUAD, QUAD * QUAD), (QUAD * QUAD) ** -0.5, 0.625, (), jnp.float32)
    recover = centred(streams_of[8], (2, QUAD * QUAD, 4 * QUAD), (4 * QUAD) ** -0.5, 1.0, (), jnp.float32)
    return {"velocity": velocity, "geometry": geometry, "element_kind": element_kind, "element_scale": element_scale, "dirichlet": dirichlet, "schur_stiffness": schur_stiffness, "schur_mass": schur_mass, "lift": lift, "recover": recover}


HIGHEST = lax.Precision.HIGHEST
SIGMA_COEF = 1.0
BETA_COEF = 0.01
STEP_DT = 0.002


def gauss_derivative(points):
    nodes = -np.cos(np.pi * (2 * np.arange(points) + 1) / (2 * points))
    ident = np.eye(points)
    diffs = nodes[:, None] - nodes[None, :] + ident
    weights = 1.0 / np.prod(diffs, axis=1)
    matrix = (weights[None, :] / weights[:, None]) / diffs
    matrix = matrix * (1.0 - ident)
    return matrix - ident * matrix.sum(axis=1)[:, None]


def kron_tables():
    deriv = gauss_derivative(QUAD)
    identity = np.eye(QUAD)
    return jnp.asarray(np.kron(deriv, identity), jnp.float32), jnp.asarray(np.kron(identity, deriv), jnp.float32)


def synthesize(coef, slope):
    planes = coef.shape[1]
    half = planes // 2
    pairs = coef[:, 1:planes - 1].reshape(coef.shape[0], half - 1, 2, coef.shape[2])
    cosine = pairs[:, :, 0]
    sine = pairs[:, :, 1]
    mean = coef[:, :1]
    top = coef[:, planes - 1:]
    if slope:
        rate = BETA_COEF * jnp.arange(1, half, dtype=jnp.float32)[None, :, None]
        cosine, sine = rate * sine, -rate * cosine
        mean = jnp.zeros_like(mean)
        top = jnp.zeros_like(top)
    real = jnp.concatenate([mean * planes, cosine * (planes / 2), top * planes], axis=1)
    imag = jnp.concatenate([jnp.zeros_like(mean), -sine * (planes / 2), jnp.zeros_like(top)], axis=1)
    return jnp.fft.irfft(lax.complex(real, imag), n=planes, axis=1)


def analyze(field):
    planes = field.shape[1]
    spectrum = jnp.fft.rfft(field, axis=1)
    real = jnp.real(spectrum)
    imag = jnp.imag(spectrum)
    mean = real[:, :1] / planes
    top = real[:, planes // 2:] / planes
    cosine = real[:, 1:planes // 2] * (2.0 / planes)
    sine = -imag[:, 1:planes // 2] * (2.0 / planes)
    pairs = jnp.stack([cosine, sine], axis=2).reshape(field.shape[0], planes - 2, field.shape[2])
    return jnp.concatenate([mean, pairs, top], axis=1)


def advect_block(coef, geo, first, second):
    values = synthesize(coef, False)
    along_z = synthesize(coef, True)
    shaped = values.reshape(3, values.shape[1], -1, QUAD * QUAD)
    along_r = jnp.einsum('cpen,mn->cpem', shaped, first, precision=HIGHEST).reshape(values.shape)
    along_s = jnp.einsum('cpen,mn->cpem', shaped, second, precision=HIGHEST).reshape(values.shape)
    along_x = geo[0] * along_r + geo[1] * along_s
    along_y = geo[2] * along_r + geo[3] * along_s
    advection = values[0] * along_x + values[1] * along_y + values[2] * along_z
    return analyze(advection)


def element_vector(vertical, horizontal):
    right = jnp.concatenate([vertical[:, :, COLUMN_ELEMS:], jnp.zeros_like(vertical[:, :, :COLUMN_ELEMS])], axis=2)
    grid = horizontal.reshape(horizontal.shape[0], horizontal.shape[1], -1, COLUMN_ELEMS)
    top = jnp.concatenate([grid[..., 1:], jnp.zeros_like(grid[..., :1])], axis=3).reshape(horizontal.shape)
    return jnp.concatenate([vertical, right, horizontal, top], axis=0)


def element_apply(vector, lam, second_kind, scale, stiffness, mass):
    flat = vector.reshape(vector.shape[0], -1)
    results = []
    for kind in range(2):
        stiff = jnp.dot(stiffness[kind], flat, precision=HIGHEST).reshape(vector.shape)
        massed = jnp.dot(mass[kind], flat, precision=HIGHEST).reshape(vector.shape)
        results.append(stiff + lam[None, :, None] * massed)
    return scale[None, None, :] * jnp.where(second_kind[None, None, :], results[1], results[0])


def assemble(outputs, free):
    left = outputs[:QUAD]
    right = outputs[QUAD:2 * QUAD]
    bottom = outputs[2 * QUAD:3 * QUAD]
    top = outputs[3 * QUAD:]
    vertical = left + jnp.concatenate([jnp.zeros_like(right[:, :, :COLUMN_ELEMS]), right[:, :, :-COLUMN_ELEMS]], axis=2)
    grid = top.reshape(top.shape[0], top.shape[1], -1, COLUMN_ELEMS)
    shifted = jnp.concatenate([jnp.zeros_like(grid[..., :1]), grid[..., :-1]], axis=3).reshape(bottom.shape)
    horizontal = bottom + shifted
    return vertical * free[0], horizontal * free[1]


def inner(first_pair, second_pair):
    return jnp.sum(first_pair[0] * second_pair[0], axis=(0, 2)) + jnp.sum(first_pair[1] * second_pair[1], axis=(0, 2))


def solve_component(comp, lam, free, second_kind, scale, stiffness, mass, lift, recover):
    planes = comp.shape[0]
    node_values = (SIGMA_COEF * comp).reshape(planes, ELEMS, QUAD * QUAD)
    lifted = jnp.where(second_kind[None, None, :],
                       jnp.einsum('kn,ren->kre', lift[1], node_values, precision=HIGHEST),
                       jnp.einsum('kn,ren->kre', lift[0], node_values, precision=HIGHEST))
    forcing = assemble(lifted, free)
    trace = (jnp.zeros_like(forcing[0]), jnp.zeros_like(forcing[1]))
    residual = forcing
    direction = forcing
    norm_now = inner(residual, residual)
    for sweep in range(CG_STEPS):
        image = assemble(element_apply(element_vector(direction[0], direction[1]), lam, second_kind, scale, stiffness, mass), free)
        alpha = (norm_now / inner(direction, image))[None, :, None]
        trace = (trace[0] + alpha * direction[0], trace[1] + alpha * direction[1])
        residual = (residual[0] - alpha * image[0], residual[1] - alpha * image[1])
        norm_next = inner(residual, residual)
        ratio = (norm_next / norm_now)[None, :, None]
        direction = (residual[0] + ratio * direction[0], residual[1] + ratio * direction[1])
        norm_now = norm_next
    vector = element_vector(trace[0], trace[1])
    recovered = jnp.where(second_kind[None, :, None],
                          jnp.einsum('nl,lre->ren', recover[1], vector, precision=HIGHEST),
                          jnp.einsum('nl,lre->ren', recover[0], vector, precision=HIGHEST))
    weight = SIGMA_COEF / (SIGMA_COEF + lam)
    return comp * weight[:, None] + recovered.reshape(comp.shape)


def reference(velocity, geometry, element_kind, element_scale, dirichlet, schur_stiffness, schur_mass, lift, recover):
    first, second = kron_tables()
    planes = velocity.shape[1]
    columns = ELEMS // COLUMN_ELEMS
    width = COLUMN_ELEMS * QUAD * QUAD
    blocks = velocity.reshape(3, planes, columns, width).transpose(2, 0, 1, 3)
    geo_blocks = geometry.reshape(4, columns, width).transpose(1, 0, 2)
    advected = lax.map(lambda pair: advect_block(pair[0], pair[1], first, second), (blocks, geo_blocks))
    advection_hat = advected.transpose(1, 2, 0, 3).reshape(velocity.shape)
    intermediate = velocity - STEP_DT * advection_hat
    waves = ((jnp.arange(planes, dtype=jnp.int32) + 1) // 2).astype(jnp.float32)
    lam = SIGMA_COEF + (BETA_COEF * waves) ** 2
    free = (1 - dirichlet).astype(jnp.float32)[:, :, None, :]
    second_kind = element_kind == 1
    return lax.map(lambda comp: solve_component(comp, lam, free, second_kind, element_scale,
                                                schur_stiffness, schur_mass, lift, recover), intermediate)
```

```python
import functools

import jax
import jax.numpy as jnp
import ml_dtypes
import numpy as np
from jax import lax
from jax.experimental import pallas as pl
from jax.experimental.pallas import tpu as pltpu
from jax.sharding import PartitionSpec as P

PLANES = 256
QUAD = 9
NODE = QUAD * QUAD
GROUPS = 64
PARTS = 4
PART_NODES = 10368
CG_STEPS = 4
BETA_COEF = 0.01
STEP_DT = 0.002
HIGHEST = lax.Precision.HIGHEST
F32 = jnp.float32
BF16 = jnp.bfloat16


def gauss_derivative(points):
    nodes = -np.cos(np.pi * (2 * np.arange(points) + 1) / (2 * points))
    ident = np.eye(points)
    diffs = nodes[:, None] - nodes[None, :] + ident
    weights = 1.0 / np.prod(diffs, axis=1)
    matrix = (weights[None, :] / weights[:, None]) / diffs
    matrix = matrix * (1.0 - ident)
    return matrix - ident * matrix.sum(axis=1)[:, None]


def split_np(table):
    high = table.astype(np.float32).astype(ml_dtypes.bfloat16)
    low = (table - high.astype(np.float64)).astype(np.float32).astype(ml_dtypes.bfloat16)
    return high, low


@functools.lru_cache(None)
def tables():
    z = np.arange(PLANES)
    rows = np.arange(PLANES).reshape(GROUPS, 4).T.reshape(-1)
    waves = (rows + 1) // 2
    angle = 2.0 * np.pi / PLANES * (waves[None, :] * z[:, None] % PLANES)
    cosine, sine = np.cos(angle), np.sin(angle)
    odd = (rows % 2 == 1)[None, :]
    ends = ((rows == 0) | (rows == PLANES - 1))[None, :]
    synth = np.where((rows == 0)[None, :], 1.0, np.where(odd, cosine, sine))
    rate = BETA_COEF * waves[None, :]
    slope = np.where(ends, 0.0, np.where(odd, -rate * sine, rate * cosine))
    weight = np.where(ends[0], 1.0 / PLANES, 2.0 / PLANES)
    analysis = synth.T * weight[:, None]
    deriv = gauss_derivative(QUAD)
    first = np.kron(deriv, np.eye(QUAD))
    second = np.kron(np.eye(QUAD), deriv)
    both = np.zeros((256, 512))
    for c in range(3):
        at = slice(c * NODE, (c + 1) * NODE)
        both[at, c * NODE:(c + 1) * NODE] = first.T
        both[at, 256 + c * NODE:256 + (c + 1) * NODE] = second.T
    out = []
    for table in (np.concatenate([synth, slope], 0), both, analysis):
        out.extend(split_np(table))
    return tuple(out)


@functools.lru_cache(None)
def selections():
    edge = np.zeros((128, 36), np.float32)
    node = np.zeros((256, NODE), np.float32)
    comp_row = np.full(128, -1)
    comp_col = np.full(256, -2)
    for c in range(3):
        for s in range(4):
            for k in range(QUAD):
                edge[s * 32 + c * QUAD + k, s * QUAD + k] = 1
                comp_row[s * 32 + c * QUAD + k] = c
        for n in range(NODE):
            node[c * NODE + n, n] = 1
            comp_col[c * NODE + n] = c
    mask_rn = (comp_row[:, None] == comp_col[None, :]).astype(np.float32)
    mask_rr = ((comp_row[:, None] == comp_row[None, :]) & (comp_row >= 0)[:, None]).astype(np.float32)
    perm = np.zeros((128, 128), np.float32)
    for p in range(GROUPS):
        for el in range(2):
            perm[2 * p + el, el * GROUPS + p] = 1
    spare = [32 * s + 27 + r for s in range(4) for r in range(5)]
    place = np.zeros((128, 24), np.float32)
    for a in range(20):
        place[spare[a], a] = 1
    pick = np.zeros((64, 128), np.float32)
    for c in range(3):
        for k in range(QUAD):
            pick[c * QUAD + k, spare[2 + k]] = 1
            pick[32 + c * QUAD + k, spare[11 + k]] = 1
    return edge, node, mask_rn, mask_rr, perm, place, pick


def split(x):
    high = x.astype(BF16)
    return high, (x - high.astype(F32)).astype(BF16)


def dot3(a, b, dims=(((1,), (0,)), ((), ()))):
    mul = functools.partial(lax.dot_general, dimension_numbers=dims, preferred_element_type=F32)
    return mul(a[0], b[0]) + (mul(a[0], b[1]) + mul(a[1], b[0]))


def dot6(a, b, dims=(((1,), (0,)), ((), ()))):
    return lax.dot_general(a, b, dims, precision=HIGHEST, preferred_element_type=F32)


NT = (((1,), (1,)), ((), ()))


def pack_kernel(v_ref, o_ref):
    lane = lax.broadcasted_iota(jnp.int32, (4, 256), 1)
    for e in range(2 * GROUPS):
        start = NODE * e
        base = min(start // 128 * 128, PART_NODES - 256)
        rows = jnp.zeros((4, 256), F32)
        for c in range(3):
            window = v_ref[c, :, base:base + 256]
            turned = pltpu.roll(window, (NODE * c - (start - base)) % 256, 1)
            rows = jnp.where((lane >= NODE * c) & (lane < NODE * (c + 1)), turned, rows)
        at = 16 * (e // 2) + 4 * (e % 2)
        o_ref[at:at + 4, :] = rows[:, :128]
        o_ref[at + 8:at + 12, :] = rows[:, 128:]


def prep_kernel(at_ref, geo_ref, kind_ref, scale_ref, dir_ref, stiff_ref, mass_ref, lift_ref, rec_ref,
                edge_ref, node_ref, mrn_ref, mrr_ref, perm_ref,
                lift_out, w_out, rec_out, geo_out, aux_out, aux_scr):
    place = at_ref[0]
    lane = lax.broadcasted_iota(jnp.int32, (4, 256), 1)
    for el in range(2):
        start = 2 * NODE * place + NODE * el
        base = pl.multiple_of(jnp.minimum(lax.div(start, 128) * 128, PART_NODES - 256), 128)
        window = geo_ref[:, pl.ds(base, 256)]
        turned = pltpu.roll(window, lax.rem(256 - (start - base), 256), 1)
        tiled = jnp.where(lane < NODE, turned,
                          jnp.where(lane < 2 * NODE, pltpu.roll(turned, NODE, 1), pltpu.roll(turned, 2 * NODE, 1)))
        geo_out[4 * el:4 * el + 4, :] = jnp.where(lane < 3 * NODE, tiled, 0.0)
    wave = lax.div(4 * place + at_ref[1] + 1, 2).astype(F32)
    lam = 1.0 + (BETA_COEF * wave) * (BETA_COEF * wave)
    edge = edge_ref[...]
    node = node_ref[...]
    for t in range(2):
        rows = slice(128 * t, 128 * (t + 1))
        lift_out[rows, :] = dot6(dot6(edge, lift_ref[t]), node, NT) * mrn_ref[...]
        rec_out[rows, :] = dot6(dot6(edge, rec_ref[t], NT), node, NT) * mrn_ref[...]
        mixed = stiff_ref[t] + lam * mass_ref[t]
        w_out[:, rows] = dot6(dot6(edge, mixed), edge, NT) * mrr_ref[...]
    second = (kind_ref[...] == 1).astype(F32)
    aux_scr[...] = jnp.zeros((24, 128), F32)
    aux_scr[0:1, :] = scale_ref[...] * (1.0 - second)
    aux_scr[1:2, :] = scale_ref[...] * second
    aux_scr[2:11, :] = (1 - dir_ref[0]).astype(F32)
    aux_scr[11:20, :] = (1 - dir_ref[1]).astype(F32)
    aux_scr[20:21, :] = second
    aux_out[...] = dot6(aux_scr[...], perm_ref[...])


def advect_kernel(x_ref, th_ref, tl_ref, dh_ref, dl_ref, ah_ref, al_ref, geo_ref, o_ref, items_scr, synth_scr, adv_scr):
    chunk = 64
    lane = lax.broadcasted_iota(jnp.int32, (chunk, 256), 1)
    low = lane < NODE
    mid = lane < 2 * NODE
    for el in range(2):
        for q in range(4):
            for t in range(2):
                items_scr[q * 64:(q + 1) * 64, t * 128:(t + 1) * 128] = x_ref[pl.ds(t * 8 + el * 4 + q, GROUPS, stride=16), :]
        synth_scr[...] = dot3((th_ref[...], tl_ref[...]), split(items_scr[...]))
        geo = geo_ref[4 * el:4 * el + 4, :]
        for at in range(0, 256, chunk):
            values = synth_scr[at:at + chunk, :]
            along_z = synth_scr[256 + at:256 + at + chunk, :]
            both = dot3(split(values), (dh_ref[...], dl_ref[...]))
            along_r = both[:, :256]
            along_s = both[:, 256:]
            along_x = geo[0:1] * along_r + geo[1:2] * along_s
            along_y = geo[2:3] * along_r + geo[3:4] * along_s
            up = pltpu.roll(values, NODE, 1)
            up2 = pltpu.roll(values, 2 * NODE, 1)
            down = pltpu.roll(values, 256 - NODE, 1)
            down2 = pltpu.roll(values, 256 - 2 * NODE, 1)
            u = jnp.where(low, values, jnp.where(mid, up, up2))
            v = jnp.where(low, down, jnp.where(mid, values, up))
            w = jnp.where(low, down2, jnp.where(mid, down, values))
            adv_scr[at:at + chunk, :] = u * along_x + v * along_y + w * along_z
        hat = dot3((ah_ref[...], al_ref[...]), split(adv_scr[...]))
        inter = items_scr[...] - STEP_DT * hat
        for q in range(4):
            for t in range(2):
                o_ref[pl.ds(t * 8 + el * 4 + q, GROUPS, stride=16), :] = inter[q * 64:(q + 1) * 64, t * 128:(t + 1) * 128]


def load_rows(x_ref, q, el, t):
    return x_ref[pl.ds(t * 8 + el * 4 + q, GROUPS, stride=16), :]


def lift_kernel(x_ref, lift_ref, aux_ref, place_ref, o_ref, in_scr):
    for q in range(4):
        for el in range(2):
            at = (2 * q + el) * 64
            for t in range(2):
                in_scr[at:at + 64, t * 128:(t + 1) * 128] = load_rows(x_ref, q, el, t)
    lifted = dot3(split(lift_ref[...]), split(in_scr[...]), NT)
    extra = dot6(place_ref[...], aux_ref[...])
    second = aux_ref[20:21, :] > 0.5
    for q in range(4):
        cols = slice(128 * q, 128 * (q + 1))
        o_ref[q] = jnp.where(second, lifted[128:, cols], lifted[:128, cols]) + extra


def turn(x, shift):
    return pltpu.roll(x, shift % 128, 1)


def cg_kernel(f_ref, w_ref, pick_ref, o_ref):
    lane = lax.broadcasted_iota(jnp.int32, (32, 128), 1)
    p = lane & 63
    el = lane >> 6
    height = 2 * (p & 15) + el
    sub = lax.broadcasted_iota(jnp.int32, (64, 1), 0) & 31
    comp = (sub >= QUAD).astype(jnp.int32) + (sub >= 2 * QUAD).astype(jnp.int32)
    zero = jnp.zeros((32, 128), F32)

    def parts(x):
        return [x[:, 128 * i:128 * (i + 1)] for i in range(PARTS)]

    def right_of(v):
        v = parts(v)
        return jnp.concatenate([jnp.where(p < 48, turn(v[i], -16), turn(v[i + 1], 48) if i < 3 else zero)
                                for i in range(PARTS)], axis=1)

    def from_left(v):
        v = parts(v)
        return jnp.concatenate([jnp.where(p >= 16, turn(v[i], 16), turn(v[i - 1], -48) if i > 0 else zero)
                                for i in range(PARTS)], axis=1)

    def top_of(h):
        return jnp.concatenate([jnp.where(height == 31, 0.0, jnp.where(el == 0, turn(x, 64), turn(x, 63)))
                                for x in parts(h)], axis=1)

    def from_below(h):
        return jnp.concatenate([jnp.where(height == 0, 0.0, jnp.where(el == 1, turn(x, 64), turn(x, -63)))
                                for x in parts(h)], axis=1)

    def vector_of(x):
        v, h = x[:32], x[32:]
        return jnp.concatenate([v, right_of(v), h, top_of(h)], axis=0)

    sent = jnp.concatenate([f_ref[i] for i in range(PARTS)], axis=1)
    free = dot6(pick_ref[...], sent)
    first_scale = sent[27:28]
    second_scale = sent[28:29]
    w = split(w_ref[...])

    def assemble(y):
        return jnp.concatenate([y[:32] + from_left(y[32:64]), y[64:96] + from_below(y[96:])], axis=0) * free

    def total(a, b):
        line = jnp.sum(a * b, axis=1, keepdims=True)
        sums = [jnp.sum(jnp.where(comp == c, line, 0.0), axis=0, keepdims=True) for c in range(3)]
        return jnp.where(comp == 0, sums[0], jnp.where(comp == 1, sums[1], sums[2]))

    residual = assemble(sent)
    direction = residual
    trace = jnp.zeros_like(residual)
    now = total(residual, residual)
    for step in range(CG_STEPS):
        vector = vector_of(direction)
        image = assemble(dot3(w, split(jnp.concatenate([vector * first_scale, vector * second_scale], axis=0))))
        alpha = now / total(direction, image)
        trace = trace + alpha * direction
        if step + 1 < CG_STEPS:
            residual = residual - alpha * image
            fresh = total(residual, residual)
            direction = residual + (fresh / now) * direction
            now = fresh
    vector = vector_of(trace)
    for i in range(PARTS):
        o_ref[i] = vector[:, 128 * i:128 * (i + 1)]


def recover_kernel(at_ref, t_ref, x_ref, rec_ref, aux_ref, o_ref, scr):
    second = aux_ref[20:21, :]
    halves = []
    for q in range(4):
        vector = t_ref[q]
        halves.append(jnp.concatenate([vector * (1.0 - second), vector * second], axis=0))
    stacked = jnp.concatenate(halves, axis=1)
    recovered = dot3(split(stacked.T), split(rec_ref[...]))
    for q in range(4):
        wave = lax.div(4 * at_ref[0] + q + 1, 2).astype(F32)
        lam = 1.0 + (BETA_COEF * wave) * (BETA_COEF * wave)
        weight = 1.0 / jnp.full((64, 128), 1.0 + lam, F32)
        for el in range(2):
            at = (2 * q + el) * 64
            for t in range(2):
                value = load_rows(x_ref, q, el, t) * weight + recovered[at:at + 64, 128 * t:128 * (t + 1)]
                scr[pl.ds(512 * t + 4 * el + q, GROUPS, stride=8), :] = value
    lane = lax.broadcasted_iota(jnp.int32, (4, 128), 1)
    for c in range(3):
        current = jnp.zeros((4, 128), F32)
        for e in range(2 * GROUPS):
            tile, offset = divmod(NODE * e, 128)
            rows = jnp.concatenate([scr[4 * e:4 * e + 4, :], scr[512 + 4 * e:516 + 4 * e, :]], axis=1)
            turned = pltpu.roll(rows, (offset - NODE * c) % 256, 1)
            current = jnp.where(lane >= offset, turned[:, :128], current)
            if offset + NODE >= 128:
                o_ref[c, :, 128 * tile:128 * (tile + 1)] = current
                current = turned[:, 128:]


VMEM = pl.BlockSpec(memory_space=pltpu.VMEM)
SMEM = pl.BlockSpec(memory_space=pltpu.SMEM)


def shape(*dims):
    return jax.ShapeDtypeStruct(dims, F32)


def call(kernel, name, out, args, scalars=0, scratch=()):
    many = isinstance(out, tuple)
    return pl.pallas_call(
        kernel,
        name=name,
        out_shape=out,
        in_specs=[SMEM] * scalars + [VMEM] * (len(args) - scalars),
        out_specs=tuple(VMEM for _ in out) if many else VMEM,
        scratch_shapes=[pltpu.VMEM(dims, F32) for dims in scratch],
    )(*args)


def exchange(value, axis, count):
    return lax.all_to_all(value.reshape(count, -1, 128), axis, split_axis=0, concat_axis=0, tiled=True)


def per_device(velocity, geometry, element_kind, element_scale, dirichlet, schur_stiffness, schur_mass, lift, recover):
    at = jnp.stack([lax.axis_index("planes"), lax.axis_index("elem")]).astype(jnp.int32)
    edge, node, mask_rn, mask_rr, perm, place, pick = selections()
    packed = call(pack_kernel, "pack", shape(1024, 128), (velocity,))
    arrived = exchange(packed, "planes", GROUPS).reshape(1024, 128)
    lift_all, w_all, rec_all, geo, aux = call(
        prep_kernel, "prep",
        (shape(256, 256), shape(128, 256), shape(256, 256), shape(8, 256), shape(24, 128)),
        (at, geometry, element_kind.reshape(1, 128), element_scale.reshape(1, 128), dirichlet,
         schur_stiffness, schur_mass, lift, recover, edge, node, mask_rn, mask_rr, perm),
        scalars=1, scratch=((24, 128),))
    inter = call(advect_kernel, "advect", shape(1024, 128), (arrived,) + tables() + (geo,),
                 scratch=((256, 256), (512, 256), (256, 256)))
    owned = exchange(inter, "planes", GROUPS).reshape(1024, 128)
    lifted = call(lift_kernel, "lift", shape(PARTS, 128, 128), (owned, lift_all, aux, place), scratch=((512, 256),))
    forcing = exchange(lifted, "elem", PARTS)
    traces = call(cg_kernel, "cg", shape(PARTS, 128, 128), (forcing, w_all, pick))
    vectors = exchange(traces, "elem", PARTS)
    return call(recover_kernel, "recover", shape(3, 4, PART_NODES), (at, vectors, owned, rec_all, aux),
                scalars=1, scratch=((1024, 128),))


def solution(mesh):
    in_specs = (
        P(None, "planes", "elem"),
        P(None, "elem"),
        P("elem"),
        P("elem"),
        P(None, None, "elem"),
        P(),
        P(),
        P(),
        P(),
    )
    out_specs = P(None, "planes", "elem")
    return jax.shard_map(per_device, mesh=mesh, in_specs=in_specs, out_specs=out_specs, check_vma=False)
```

```python
import functools

import jax
import jax.numpy as jnp
import ml_dtypes
import numpy as np
from jax import lax
from jax.experimental import pallas as pl
from jax.experimental.pallas import tpu as pltpu
from jax.sharding import PartitionSpec as P

PLANES = 256
QUAD = 9
NODE = QUAD * QUAD
GROUPS = 64
PARTS = 4
PART_NODES = 10368
CG_STEPS = 4
BETA_COEF = 0.01
STEP_DT = 0.002
HIGHEST = lax.Precision.HIGHEST
F32 = jnp.float32
BF16 = jnp.bfloat16


def gauss_derivative(points):
    nodes = -np.cos(np.pi * (2 * np.arange(points) + 1) / (2 * points))
    ident = np.eye(points)
    diffs = nodes[:, None] - nodes[None, :] + ident
    weights = 1.0 / np.prod(diffs, axis=1)
    matrix = (weights[None, :] / weights[:, None]) / diffs
    matrix = matrix * (1.0 - ident)
    return matrix - ident * matrix.sum(axis=1)[:, None]


def split_np(table):
    high = table.astype(np.float32).astype(ml_dtypes.bfloat16)
    low = (table - high.astype(np.float64)).astype(np.float32).astype(ml_dtypes.bfloat16)
    return high, low


@functools.lru_cache(None)
def tables():
    z = np.arange(PLANES)
    rows = np.arange(PLANES).reshape(GROUPS, 4).T.reshape(-1)
    waves = (rows + 1) // 2
    angle = 2.0 * np.pi / PLANES * (waves[None, :] * z[:, None] % PLANES)
    cosine, sine = np.cos(angle), np.sin(angle)
    odd = (rows % 2 == 1)[None, :]
    ends = ((rows == 0) | (rows == PLANES - 1))[None, :]
    synth = np.where((rows == 0)[None, :], 1.0, np.where(odd, cosine, sine))
    rate = BETA_COEF * waves[None, :]
    slope = np.where(ends, 0.0, np.where(odd, -rate * sine, rate * cosine))
    weight = np.where(ends[0], 1.0 / PLANES, 2.0 / PLANES)
    analysis = synth.T * weight[:, None]
    deriv = gauss_derivative(QUAD)
    first = np.kron(deriv, np.eye(QUAD))
    second = np.kron(np.eye(QUAD), deriv)
    both = np.zeros((256, 512))
    for c in range(3):
        at = slice(c * NODE, (c + 1) * NODE)
        both[at, c * NODE:(c + 1) * NODE] = first.T
        both[at, 256 + c * NODE:256 + (c + 1) * NODE] = second.T
    out = []
    for table in (np.concatenate([synth, slope], 0), both, analysis):
        out.extend(split_np(table))
    return tuple(out)


@functools.lru_cache(None)
def selections():
    edge = np.zeros((128, 36), np.float32)
    node = np.zeros((256, NODE), np.float32)
    comp_row = np.full(128, -1)
    comp_col = np.full(256, -2)
    for c in range(3):
        for s in range(4):
            for k in range(QUAD):
                edge[s * 32 + c * QUAD + k, s * QUAD + k] = 1
                comp_row[s * 32 + c * QUAD + k] = c
        for n in range(NODE):
            node[c * NODE + n, n] = 1
            comp_col[c * NODE + n] = c
    mask_rn = (comp_row[:, None] == comp_col[None, :]).astype(np.float32)
    mask_rr = ((comp_row[:, None] == comp_row[None, :]) & (comp_row >= 0)[:, None]).astype(np.float32)
    perm = np.zeros((128, 128), np.float32)
    for p in range(GROUPS):
        for el in range(2):
            perm[2 * p + el, el * GROUPS + p] = 1
    spare = [32 * s + 27 + r for s in range(4) for r in range(5)]
    place = np.zeros((128, 24), np.float32)
    for a in range(20):
        place[spare[a], a] = 1
    pick = np.zeros((64, 128), np.float32)
    for c in range(3):
        for k in range(QUAD):
            pick[c * QUAD + k, spare[2 + k]] = 1
            pick[32 + c * QUAD + k, spare[11 + k]] = 1
    return edge, node, mask_rn, mask_rr, perm, place, pick


def split(x):
    high = x.astype(BF16)
    return high, (x - high.astype(F32)).astype(BF16)


def dot3(a, b, dims=(((1,), (0,)), ((), ()))):
    mul = functools.partial(lax.dot_general, dimension_numbers=dims, preferred_element_type=F32)
    return mul(a[0], b[0]) + (mul(a[0], b[1]) + mul(a[1], b[0]))


def dot6(a, b, dims=(((1,), (0,)), ((), ()))):
    return lax.dot_general(a, b, dims, precision=HIGHEST, preferred_element_type=F32)


NT = (((1,), (1,)), ((), ()))


def pack_kernel(v_ref, o_ref):
    lane = lax.broadcasted_iota(jnp.int32, (4, 256), 1)
    for e in range(2 * GROUPS):
        start = NODE * e
        base = min(start // 128 * 128, PART_NODES - 256)
        rows = jnp.zeros((4, 256), F32)
        for c in range(3):
            window = v_ref[c, :, base:base + 256]
            turned = pltpu.roll(window, (NODE * c - (start - base)) % 256, 1)
            rows = jnp.where((lane >= NODE * c) & (lane < NODE * (c + 1)), turned, rows)
        at = 16 * (e // 2) + 4 * (e % 2)
        o_ref[at:at + 4, :] = rows[:, :128]
        o_ref[at + 8:at + 12, :] = rows[:, 128:]


def prep_kernel(at_ref, geo_ref, kind_ref, scale_ref, dir_ref, stiff_ref, mass_ref, lift_ref, rec_ref,
                edge_ref, node_ref, mrn_ref, mrr_ref, perm_ref,
                lift_out, w_out, rec_out, geo_out, aux_out, aux_scr):
    place = at_ref[0]
    lane = lax.broadcasted_iota(jnp.int32, (4, 256), 1)
    for el in range(2):
        start = 2 * NODE * place + NODE * el
        base = pl.multiple_of(jnp.minimum(lax.div(start, 128) * 128, PART_NODES - 256), 128)
        window = geo_ref[:, pl.ds(base, 256)]
        turned = pltpu.roll(window, lax.rem(256 - (start - base), 256), 1)
        tiled = jnp.where(lane < NODE, turned,
                          jnp.where(lane < 2 * NODE, pltpu.roll(turned, NODE, 1), pltpu.roll(turned, 2 * NODE, 1)))
        geo_out[4 * el:4 * el + 4, :] = jnp.where(lane < 3 * NODE, tiled, 0.0)
    wave = lax.div(4 * place + at_ref[1] + 1, 2).astype(F32)
    lam = 1.0 + (BETA_COEF * wave) * (BETA_COEF * wave)
    edge = edge_ref[...]
    node = node_ref[...]
    for t in range(2):
        rows = slice(128 * t, 128 * (t + 1))
        lift_out[rows, :] = dot6(dot6(edge, lift_ref[t]), node, NT) * mrn_ref[...]
        rec_out[rows, :] = dot6(dot6(edge, rec_ref[t], NT), node, NT) * mrn_ref[...]
        mixed = stiff_ref[t] + lam * mass_ref[t]
        w_out[:, rows] = dot6(dot6(edge, mixed), edge, NT) * mrr_ref[...]
    second = (kind_ref[...] == 1).astype(F32)
    aux_scr[...] = jnp.zeros((24, 128), F32)
    aux_scr[0:1, :] = scale_ref[...] * (1.0 - second)
    aux_scr[1:2, :] = scale_ref[...] * second
    aux_scr[2:11, :] = (1 - dir_ref[0]).astype(F32)
    aux_scr[11:20, :] = (1 - dir_ref[1]).astype(F32)
    aux_scr[20:21, :] = second
    aux_out[...] = dot6(aux_scr[...], perm_ref[...])


def advect_kernel(x_ref, th_ref, tl_ref, dh_ref, dl_ref, ah_ref, al_ref, geo_ref, o_ref, items_scr, synth_scr, adv_scr):
    chunk = 64
    lane = lax.broadcasted_iota(jnp.int32, (chunk, 256), 1)
    low = lane < NODE
    mid = lane < 2 * NODE
    for el in range(2):
        for q in range(4):
            for t in range(2):
                items_scr[q * 64:(q + 1) * 64, t * 128:(t + 1) * 128] = x_ref[pl.ds(t * 8 + el * 4 + q, GROUPS, stride=16), :]
        synth_scr[...] = dot3((th_ref[...], tl_ref[...]), split(items_scr[...]))
        geo = geo_ref[4 * el:4 * el + 4, :]
        for at in range(0, 256, chunk):
            values = synth_scr[at:at + chunk, :]
            along_z = synth_scr[256 + at:256 + at + chunk, :]
            both = dot3(split(values), (dh_ref[...], dl_ref[...]))
            along_r = both[:, :256]
            along_s = both[:, 256:]
            along_x = geo[0:1] * along_r + geo[1:2] * along_s
            along_y = geo[2:3] * along_r + geo[3:4] * along_s
            up = pltpu.roll(values, NODE, 1)
            up2 = pltpu.roll(values, 2 * NODE, 1)
            down = pltpu.roll(values, 256 - NODE, 1)
            down2 = pltpu.roll(values, 256 - 2 * NODE, 1)
            u = jnp.where(low, values, jnp.where(mid, up, up2))
            v = jnp.where(low, down, jnp.where(mid, values, up))
            w = jnp.where(low, down2, jnp.where(mid, down, values))
            adv_scr[at:at + chunk, :] = u * along_x + v * along_y + w * along_z
        hat = dot3((ah_ref[...], al_ref[...]), split(adv_scr[...]))
        inter = items_scr[...] - STEP_DT * hat
        for q in range(4):
            for t in range(2):
                o_ref[pl.ds(t * 8 + el * 4 + q, GROUPS, stride=16), :] = inter[q * 64:(q + 1) * 64, t * 128:(t + 1) * 128]


def load_rows(x_ref, q, el, t):
    return x_ref[pl.ds(t * 8 + el * 4 + q, GROUPS, stride=16), :]


def lift_kernel(at_ref, x_ref, lift_ref, aux_ref, place_ref, o0_ref, o1_ref, o2_ref, o3_ref, in_scr, out_scr):
    for q in range(4):
        for el in range(2):
            at = (2 * q + el) * 64
            for t in range(2):
                in_scr[at:at + 64, t * 128:(t + 1) * 128] = load_rows(x_ref, q, el, t)
    lifted = dot3(split(lift_ref[...]), split(in_scr[...]), NT)
    extra = dot6(place_ref[...], aux_ref[...])
    second = aux_ref[20:21, :] > 0.5
    for q in range(4):
        cols = slice(128 * q, 128 * (q + 1))
        out_scr[q] = jnp.where(second, lifted[128:, cols], lifted[:128, cols]) + extra
    for k, ref in enumerate((o0_ref, o1_ref, o2_ref, o3_ref)):
        ref[...] = out_scr[lax.rem(at_ref[1] + k, PARTS)]


def turn(x, shift):
    return pltpu.roll(x, shift % 128, 1)


def cg_kernel(at_ref, f0_ref, f1_ref, f2_ref, f3_ref, w_ref, pick_ref, o0_ref, o1_ref, o2_ref, o3_ref, scr):
    for k, ref in enumerate((f0_ref, f1_ref, f2_ref, f3_ref)):
        scr[lax.rem(at_ref[1] + PARTS - k, PARTS)] = ref[...]
    lane = lax.broadcasted_iota(jnp.int32, (32, 128), 1)
    p = lane & 63
    el = lane >> 6
    height = 2 * (p & 15) + el
    sub = lax.broadcasted_iota(jnp.int32, (64, 1), 0) & 31
    comp = (sub >= QUAD).astype(jnp.int32) + (sub >= 2 * QUAD).astype(jnp.int32)
    zero = jnp.zeros((32, 128), F32)

    def parts(x):
        return [x[:, 128 * i:128 * (i + 1)] for i in range(PARTS)]

    def right_of(v):
        v = parts(v)
        return jnp.concatenate([jnp.where(p < 48, turn(v[i], -16), turn(v[i + 1], 48) if i < 3 else zero)
                                for i in range(PARTS)], axis=1)

    def from_left(v):
        v = parts(v)
        return jnp.concatenate([jnp.where(p >= 16, turn(v[i], 16), turn(v[i - 1], -48) if i > 0 else zero)
                                for i in range(PARTS)], axis=1)

    def top_of(h):
        return jnp.concatenate([jnp.where(height == 31, 0.0, jnp.where(el == 0, turn(x, 64), turn(x, 63)))
                                for x in parts(h)], axis=1)

    def from_below(h):
        return jnp.concatenate([jnp.where(height == 0, 0.0, jnp.where(el == 1, turn(x, 64), turn(x, -63)))
                                for x in parts(h)], axis=1)

    def vector_of(x):
        v, h = x[:32], x[32:]
        return jnp.concatenate([v, right_of(v), h, top_of(h)], axis=0)

    sent = jnp.concatenate([scr[i] for i in range(PARTS)], axis=1)
    free = dot6(pick_ref[...], sent)
    first_scale = sent[27:28]
    second_scale = sent[28:29]
    w = split(w_ref[...])

    def assemble(y):
        return jnp.concatenate([y[:32] + from_left(y[32:64]), y[64:96] + from_below(y[96:])], axis=0) * free

    def total(a, b):
        line = jnp.sum(a * b, axis=1, keepdims=True)
        sums = [jnp.sum(jnp.where(comp == c, line, 0.0), axis=0, keepdims=True) for c in range(3)]
        return jnp.where(comp == 0, sums[0], jnp.where(comp == 1, sums[1], sums[2]))

    residual = assemble(sent)
    direction = residual
    trace = jnp.zeros_like(residual)
    now = total(residual, residual)
    for step in range(CG_STEPS):
        vector = vector_of(direction)
        image = assemble(dot3(w, split(jnp.concatenate([vector * first_scale, vector * second_scale], axis=0))))
        alpha = now / total(direction, image)
        trace = trace + alpha * direction
        if step + 1 < CG_STEPS:
            residual = residual - alpha * image
            fresh = total(residual, residual)
            direction = residual + (fresh / now) * direction
            now = fresh
    vector = vector_of(trace)
    for i in range(PARTS):
        scr[i] = vector[:, 128 * i:128 * (i + 1)]
    for k, ref in enumerate((o0_ref, o1_ref, o2_ref, o3_ref)):
        ref[...] = scr[lax.rem(at_ref[1] + k, PARTS)]


def recover_kernel(at_ref, t0_ref, t1_ref, t2_ref, t3_ref, x_ref, rec_ref, aux_ref, o_ref, scr, t_scr):
    for k, ref in enumerate((t0_ref, t1_ref, t2_ref, t3_ref)):
        t_scr[lax.rem(at_ref[1] + PARTS - k, PARTS)] = ref[...]
    second = aux_ref[20:21, :]
    halves = []
    for q in range(4):
        vector = t_scr[q]
        halves.append(jnp.concatenate([vector * (1.0 - second), vector * second], axis=0))
    stacked = jnp.concatenate(halves, axis=1)
    recovered = dot3(split(stacked.T), split(rec_ref[...]))
    for q in range(4):
        wave = lax.div(4 * at_ref[0] + q + 1, 2).astype(F32)
        lam = 1.0 + (BETA_COEF * wave) * (BETA_COEF * wave)
        weight = 1.0 / jnp.full((64, 128), 1.0 + lam, F32)
        for el in range(2):
            at = (2 * q + el) * 64
            for t in range(2):
                value = load_rows(x_ref, q, el, t) * weight + recovered[at:at + 64, 128 * t:128 * (t + 1)]
                scr[pl.ds(512 * t + 4 * el + q, GROUPS, stride=8), :] = value
    lane = lax.broadcasted_iota(jnp.int32, (4, 128), 1)
    for c in range(3):
        current = jnp.zeros((4, 128), F32)
        for e in range(2 * GROUPS):
            tile, offset = divmod(NODE * e, 128)
            rows = jnp.concatenate([scr[4 * e:4 * e + 4, :], scr[512 + 4 * e:516 + 4 * e, :]], axis=1)
            turned = pltpu.roll(rows, (offset - NODE * c) % 256, 1)
            current = jnp.where(lane >= offset, turned[:, :128], current)
            if offset + NODE >= 128:
                o_ref[c, :, 128 * tile:128 * (tile + 1)] = current
                current = turned[:, 128:]


VMEM = pl.BlockSpec(memory_space=pltpu.VMEM)
SMEM = pl.BlockSpec(memory_space=pltpu.SMEM)


def shape(*dims):
    return jax.ShapeDtypeStruct(dims, F32)


def call(kernel, name, out, args, scalars=0, scratch=(), near=True):
    many = isinstance(out, tuple)
    args = args[:scalars] + tuple(pltpu.with_memory_space_constraint(jnp.asarray(a), pltpu.VMEM) for a in args[scalars:])
    if near:
        outs = tuple(pltpu.VMEM(o.shape, F32) for o in (out if many else (out,)))
        out = outs if many else outs[0]
    return pl.pallas_call(
        kernel,
        name=name,
        out_shape=out,
        in_specs=[SMEM] * scalars + [VMEM] * (len(args) - scalars),
        out_specs=tuple(VMEM for _ in out) if many else VMEM,
        scratch_shapes=[pltpu.VMEM(dims, F32) for dims in scratch],
    )(*args)


def exchange(value, axis, count):
    return lax.all_to_all(value.reshape(count, -1, 128), axis, split_axis=0, concat_axis=0, tiled=True)


def spread(blocks):
    moved = [lax.ppermute(blocks[k], "elem", [(s, (s + k) % PARTS) for s in range(PARTS)]) for k in range(1, PARTS)]
    return (blocks[0],) + tuple(moved)


def per_device(velocity, geometry, element_kind, element_scale, dirichlet, schur_stiffness, schur_mass, lift, recover):
    at = jnp.stack([lax.axis_index("planes"), lax.axis_index("elem")]).astype(jnp.int32)
    edge, node, mask_rn, mask_rr, perm, place, pick = selections()
    packed = call(pack_kernel, "pack", shape(1024, 128), (velocity,))
    arrived = exchange(packed, "planes", GROUPS).reshape(1024, 128)
    lift_all, w_all, rec_all, geo, aux = call(
        prep_kernel, "prep",
        (shape(256, 256), shape(128, 256), shape(256, 256), shape(8, 256), shape(24, 128)),
        (at, geometry, element_kind.reshape(1, 128), element_scale.reshape(1, 128), dirichlet,
         schur_stiffness, schur_mass, lift, recover, edge, node, mask_rn, mask_rr, perm),
        scalars=1, scratch=((24, 128),))
    inter = call(advect_kernel, "advect", shape(1024, 128), (arrived,) + tables() + (geo,),
                 scratch=((256, 256), (512, 256), (256, 256)))
    owned = exchange(inter, "planes", GROUPS).reshape(1024, 128)
    block = shape(128, 128)
    lifted = call(lift_kernel, "lift", (block,) * PARTS, (at, owned, lift_all, aux, place), scalars=1,
                  scratch=((512, 256), (PARTS, 128, 128)))
    traces = call(cg_kernel, "cg", (block,) * PARTS, (at,) + spread(lifted) + (w_all, pick), scalars=1,
                  scratch=((PARTS, 128, 128),))
    return call(recover_kernel, "recover", shape(3, 4, PART_NODES), (at,) + spread(traces) + (owned, rec_all, aux),
                scalars=1, scratch=((1024, 128), (PARTS, 128, 128)), near=False)


def solution(mesh):
    in_specs = (
        P(None, "planes", "elem"),
        P(None, "elem"),
        P("elem"),
        P("elem"),
        P(None, None, "elem"),
        P(),
        P(),
        P(),
        P(),
    )
    out_specs = P(None, "planes", "elem")
    return jax.shard_map(per_device, mesh=mesh, in_specs=in_specs, out_specs=out_specs, check_vma=False)
```

```python
import functools

import jax
import jax.numpy as jnp
import ml_dtypes
import numpy as np
from jax import lax
from jax.experimental import pallas as pl
from jax.experimental.pallas import tpu as pltpu
from jax.sharding import PartitionSpec as P

PLANES = 256
QUAD = 9
NODE = QUAD * QUAD
GROUPS = 64
PARTS = 4
PART_NODES = 10368
CG_STEPS = 4
BETA_COEF = 0.01
STEP_DT = 0.002
HIGHEST = lax.Precision.HIGHEST
F32 = jnp.float32
BF16 = jnp.bfloat16


def gauss_derivative(points):
    nodes = -np.cos(np.pi * (2 * np.arange(points) + 1) / (2 * points))
    ident = np.eye(points)
    diffs = nodes[:, None] - nodes[None, :] + ident
    weights = 1.0 / np.prod(diffs, axis=1)
    matrix = (weights[None, :] / weights[:, None]) / diffs
    matrix = matrix * (1.0 - ident)
    return matrix - ident * matrix.sum(axis=1)[:, None]


def split_np(table):
    high = table.astype(np.float32).astype(ml_dtypes.bfloat16)
    low = (table - high.astype(np.float64)).astype(np.float32).astype(ml_dtypes.bfloat16)
    return high, low


@functools.lru_cache(None)
def tables():
    z = np.arange(PLANES)
    rows = np.arange(PLANES)
    waves = (rows + 1) // 2
    angle = 2.0 * np.pi / PLANES * (waves[None, :] * z[:, None] % PLANES)
    cosine, sine = np.cos(angle), np.sin(angle)
    odd = (rows % 2 == 1)[None, :]
    ends = ((rows == 0) | (rows == PLANES - 1))[None, :]
    synth = np.where((rows == 0)[None, :], 1.0, np.where(odd, cosine, sine))
    rate = BETA_COEF * waves[None, :]
    slope = np.where(ends, 0.0, np.where(odd, -rate * sine, rate * cosine))
    weight = np.where(ends[0], 1.0 / PLANES, 2.0 / PLANES)
    analysis = synth.T * weight[:, None]
    deriv = gauss_derivative(QUAD)
    first = np.kron(deriv, np.eye(QUAD))
    second = np.kron(np.eye(QUAD), deriv)
    both = np.zeros((256, 512))
    for c in range(3):
        at = slice(c * NODE, (c + 1) * NODE)
        both[at, c * NODE:(c + 1) * NODE] = first.T
        both[at, 256 + c * NODE:256 + (c + 1) * NODE] = second.T
    out = []
    for table in (np.concatenate([synth, slope], 0), both, analysis):
        out.extend(split_np(table))
    return tuple(out)


@functools.lru_cache(None)
def selections():
    edge = np.zeros((128, 36), np.float32)
    node = np.zeros((256, NODE), np.float32)
    comp_row = np.full(128, -1)
    comp_col = np.full(256, -2)
    for c in range(3):
        for s in range(4):
            for k in range(QUAD):
                edge[s * 32 + c * QUAD + k, s * QUAD + k] = 1
                comp_row[s * 32 + c * QUAD + k] = c
        for n in range(NODE):
            node[c * NODE + n, n] = 1
            comp_col[c * NODE + n] = c
    mask_rn = (comp_row[:, None] == comp_col[None, :]).astype(np.float32)
    mask_rr = ((comp_row[:, None] == comp_row[None, :]) & (comp_row >= 0)[:, None]).astype(np.float32)
    perm = np.zeros((128, 128), np.float32)
    for p in range(GROUPS):
        for el in range(2):
            perm[2 * p + el, el * GROUPS + p] = 1
    pick = np.zeros((64, 24), np.float32)
    for c in range(3):
        for k in range(QUAD):
            pick[c * QUAD + k, 2 + k] = 1
            pick[32 + c * QUAD + k, 11 + k] = 1
    return edge, node, mask_rn, mask_rr, perm, pick


def split(x):
    high = x.astype(BF16)
    return high, (x - high.astype(F32)).astype(BF16)


def dot3(a, b, dims=(((1,), (0,)), ((), ()))):
    mul = functools.partial(lax.dot_general, dimension_numbers=dims, preferred_element_type=F32)
    return mul(a[0], b[0]) + (mul(a[0], b[1]) + mul(a[1], b[0]))


def dot6(a, b, dims=(((1,), (0,)), ((), ()))):
    return lax.dot_general(a, b, dims, precision=HIGHEST, preferred_element_type=F32)


NT = (((1,), (1,)), ((), ()))


PACK_STEPS = 2
PACK_ELEMS = 2 * GROUPS // PACK_STEPS


def window_base(e):
    return min(NODE * e // 128 * 128, PART_NODES - 256)


PACK_CUTS = (0,) + tuple(window_base(PACK_ELEMS * (g + 1) - 1) + 256 for g in range(PACK_STEPS))


def pack_kernel(v_ref, o_ref, v_scr, o_scr, in_sems, out_sems):
    lane = lax.broadcasted_iota(jnp.int32, (4, 256), 1)

    def arriving(g):
        cols = slice(PACK_CUTS[g], PACK_CUTS[g + 1])
        return pltpu.make_async_copy(v_ref.at[:, :, cols], v_scr.at[:, :, cols], in_sems.at[g])

    def leaving(g):
        rows = slice(8 * PACK_ELEMS * g, 8 * PACK_ELEMS * (g + 1))
        return pltpu.make_async_copy(o_scr.at[rows], o_ref.at[rows], out_sems.at[g])

    for g in range(PACK_STEPS):
        arriving(g).start()
    for g in range(PACK_STEPS):
        arriving(g).wait()
        for e in range(PACK_ELEMS * g, PACK_ELEMS * (g + 1)):
            start = NODE * e
            base = window_base(e)
            rows = jnp.zeros((4, 256), F32)
            for c in range(3):
                window = v_scr[c, :, base:base + 256]
                turned = pltpu.roll(window, (NODE * c - (start - base)) % 256, 1)
                rows = jnp.where((lane >= NODE * c) & (lane < NODE * (c + 1)), turned, rows)
            at = 16 * (e // 2) + 4 * (e % 2)
            o_scr[at:at + 4, :] = rows[:, :128]
            o_scr[at + 8:at + 12, :] = rows[:, 128:]
        leaving(g).start()
    for g in range(PACK_STEPS):
        leaving(g).wait()


def prep_kernel(geo_ref, kind_ref, scale_ref, dir_ref, stiff_ref, mass_ref, lift_ref, rec_ref,
                edge_ref, node_ref, mrn_ref, mrr_ref, perm_ref,
                lift_out, w_out, rec_out, geo_out, aux_out, aux_scr):
    place = lax.axis_index("planes")
    lane = lax.broadcasted_iota(jnp.int32, (4, 256), 1)
    for el in range(2):
        start = 2 * NODE * place + NODE * el
        base = pl.multiple_of(jnp.minimum(lax.div(start, 128) * 128, PART_NODES - 256), 128)
        window = geo_ref[:, pl.ds(base, 256)]
        turned = pltpu.roll(window, lax.rem(256 - (start - base), 256), 1)
        tiled = jnp.where(lane < NODE, turned,
                          jnp.where(lane < 2 * NODE, pltpu.roll(turned, NODE, 1), pltpu.roll(turned, 2 * NODE, 1)))
        geo_out[4 * el:4 * el + 4, :] = jnp.where(lane < 3 * NODE, tiled, 0.0)
    wave = lax.div(4 * place + lax.axis_index("elem") + 1, 2).astype(F32)
    lam = 1.0 + (BETA_COEF * wave) * (BETA_COEF * wave)
    edge = edge_ref[...]
    node = node_ref[...]
    for t in range(2):
        rows = slice(128 * t, 128 * (t + 1))
        lift_out[rows, :] = dot6(dot6(edge, lift_ref[t]), node, NT) * mrn_ref[...]
        rec_out[rows, :] = dot6(dot6(edge, rec_ref[t], NT), node, NT) * mrn_ref[...]
        mixed = stiff_ref[t] + lam * mass_ref[t]
        w_out[:, rows] = dot6(dot6(edge, mixed), edge, NT) * mrr_ref[...]
    second = (kind_ref[...] == 1).astype(F32)
    aux_scr[...] = jnp.zeros((24, 128), F32)
    aux_scr[0:1, :] = scale_ref[...] * (1.0 - second)
    aux_scr[1:2, :] = scale_ref[...] * second
    aux_scr[2:11, :] = (1 - dir_ref[0]).astype(F32)
    aux_scr[11:20, :] = (1 - dir_ref[1]).astype(F32)
    aux_scr[20:21, :] = second
    aux_out[...] = dot6(aux_scr[...], perm_ref[...])


def swap_halves(x, y):
    first = lax.broadcasted_iota(jnp.int32, x.shape, 1) < 4
    return jnp.where(first, x, pltpu.roll(y, 4, 1)), jnp.where(first, pltpu.roll(x, 4, 1), y)


def advect_kernel(x_ref, th_ref, tl_ref, dh_ref, dl_ref, ah_ref, al_ref, geo_ref, o_ref, items_scr, synth_scr, adv_scr):
    lane = lax.broadcasted_iota(jnp.int32, (256, 256), 1)
    low = lane < NODE
    mid = lane < 2 * NODE
    for t in range(2):
        pairs = [jnp.concatenate([x_ref[32 * m + 16 * odd + 8 * t:32 * m + 16 * odd + 8 * t + 8, :] for m in range(32)], axis=0)
                 .reshape(32, 8, 128) for odd in range(2)]
        for el, rows in enumerate(swap_halves(*pairs)):
            items_scr[256 * el:256 * (el + 1), 128 * t:128 * (t + 1)] = rows.reshape(256, 128)
    for el in range(2):
        here = slice(256 * el, 256 * (el + 1))
        synth_scr[...] = dot3((th_ref[...], tl_ref[...]), split(items_scr[here, :]))
        geo = geo_ref[4 * el:4 * el + 4, :]
        values = synth_scr[:256, :]
        both = dot3(split(values), (dh_ref[...], dl_ref[...]))
        along_r = both[:, :256]
        along_s = both[:, 256:]
        along_x = geo[0:1] * along_r + geo[1:2] * along_s
        along_y = geo[2:3] * along_r + geo[3:4] * along_s
        up = pltpu.roll(values, NODE, 1)
        up2 = pltpu.roll(values, 2 * NODE, 1)
        down = pltpu.roll(values, 256 - NODE, 1)
        down2 = pltpu.roll(values, 256 - 2 * NODE, 1)
        u = jnp.where(low, values, jnp.where(mid, up, up2))
        v = jnp.where(low, down, jnp.where(mid, values, up))
        w = jnp.where(low, down2, jnp.where(mid, down, values))
        adv_scr[...] = u * along_x + v * along_y + w * synth_scr[256:, :]
        hat = dot3((ah_ref[...], al_ref[...]), split(adv_scr[...]))
        items_scr[here, :] = items_scr[here, :] - STEP_DT * hat
    for t in range(2):
        elems = [items_scr[256 * el:256 * (el + 1), 128 * t:128 * (t + 1)].reshape(32, 8, 128) for el in range(2)]
        for odd, rows in enumerate(swap_halves(*elems)):
            for m in range(32):
                at = 32 * m + 16 * odd + 8 * t
                o_ref[at:at + 8, :] = rows[m]


def turn(x, shift):
    return pltpu.roll(x, shift % 128, 1)


def lanes(rows):
    lane = lax.broadcasted_iota(jnp.int32, (rows, 128), 1)
    p = lane & 63
    el = lane >> 6
    return p, el, 2 * (p & 15) + el


def fold(x, first):
    group = lanes(8)[0] >> 4
    out = jnp.zeros((8, 128), F32)
    for g in range(4):
        out = jnp.where(group == g, turn(x[8 * g:8 * g + 8], 16 * g - first), out)
    return out


def unfold(x, first):
    return jnp.concatenate([turn(x, first - 16 * g) for g in range(4)], axis=0)


def take_top(h):
    p, el, height = lanes(32)
    return jnp.where(height == 31, 0.0, jnp.where(el == 0, turn(h, 64), turn(h, 63)))


def give_top(h):
    p, el, height = lanes(32)
    return jnp.where(height == 0, 0.0, jnp.where(el == 1, turn(h, 64), turn(h, -63)))


def lift_kernel(x_ref, lift_ref, aux_ref, o0_ref, o1_ref, o2_ref, o3_ref, in_scr, out_scr):
    arrived = jnp.transpose(x_ref[...].reshape(GROUPS, 16, 128), (1, 0, 2))
    for q in range(4):
        for el in range(2):
            at = (2 * q + el) * 64
            for t in range(2):
                in_scr[at:at + 64, t * 128:(t + 1) * 128] = arrived[t * 8 + el * 4 + q]
    lifted = dot3(split(lift_ref[...]), split(in_scr[...]), NT)
    second = aux_ref[20:21, :] > 0.5
    p = lanes(32)[0]
    for q in range(4):
        cols = slice(128 * q, 128 * (q + 1))
        edges = jnp.where(second, lifted[128:, cols], lifted[:128, cols])
        right = edges[32:64]
        out_scr[q, 0:32] = edges[0:32] + jnp.where(p >= 16, turn(right, 16), 0.0)
        out_scr[q, 32:64] = edges[64:96] + give_top(edges[96:128])
        out_scr[q, 64:72] = fold(right, 48)
        out_scr[q, 72:96] = aux_ref[...]
    for k, ref in enumerate((o0_ref, o1_ref, o2_ref, o3_ref)):
        ref[...] = out_scr[lax.rem(lax.axis_index("elem") + k, PARTS)]


def cg_kernel(f0_ref, f1_ref, f2_ref, f3_ref, w_ref, pick_ref, o0_ref, o1_ref, o2_ref, o3_ref, scr):
    for k, ref in enumerate((f0_ref, f1_ref, f2_ref, f3_ref)):
        scr[lax.rem(lax.axis_index("elem") + PARTS - k, PARTS)] = ref[...]
    p = lanes(32)[0]
    sub = lax.broadcasted_iota(jnp.int32, (64, 1), 0) & 31
    comp = (sub >= QUAD).astype(jnp.int32) + (sub >= 2 * QUAD).astype(jnp.int32)
    zero = jnp.zeros((32, 128), F32)

    def parts(x):
        return [x[:, 128 * i:128 * (i + 1)] for i in range(PARTS)]

    def right_of(v):
        v = parts(v)
        return jnp.concatenate([jnp.where(p < 48, turn(v[i], -16), turn(v[i + 1], 48) if i < 3 else zero)
                                for i in range(PARTS)], axis=1)

    def from_left(v):
        v = parts(v)
        return jnp.concatenate([jnp.where(p >= 16, turn(v[i], 16), turn(v[i - 1], -48) if i > 0 else zero)
                                for i in range(PARTS)], axis=1)

    def top_of(h):
        return jnp.concatenate([take_top(x) for x in parts(h)], axis=1)

    def from_below(h):
        return jnp.concatenate([give_top(x) for x in parts(h)], axis=1)

    def vector_of(x):
        v, h = x[:32], x[32:]
        return jnp.concatenate([v, right_of(v), h, top_of(h)], axis=0)

    aux = jnp.concatenate([scr[i, 72:96] for i in range(PARTS)], axis=1)
    free = dot6(pick_ref[...], aux)
    first_scale = aux[0:1]
    second_scale = aux[1:2]
    w_high, w_low = split(w_ref[...])
    w_both = jnp.concatenate([w_high, w_low], axis=0)

    def operator(x):
        high, low = split(x)
        both = lax.dot(w_both, high, preferred_element_type=F32)
        return both[:128] + (both[128:] + lax.dot(w_high, low, preferred_element_type=F32))

    def assemble(y):
        return jnp.concatenate([y[:32] + from_left(y[32:64]), y[64:96] + from_below(y[96:])], axis=0) * free

    def total(a, b):
        line = jnp.sum(a * b, axis=1, keepdims=True)
        sums = [jnp.sum(jnp.where(comp == c, line, 0.0), axis=0, keepdims=True) for c in range(3)]
        return jnp.where(comp == 0, sums[0], jnp.where(comp == 1, sums[1], sums[2]))

    sent = []
    for i in range(PARTS):
        v = scr[i, 0:32]
        if i > 0:
            v = v + jnp.where(p < 16, unfold(scr[i - 1, 64:72], 0), 0.0)
        sent.append(jnp.concatenate([v, scr[i, 32:64]], axis=0))
    residual = jnp.concatenate(sent, axis=1) * free
    direction = residual
    trace = jnp.zeros_like(residual)
    now = total(residual, residual)
    for step in range(CG_STEPS):
        vector = vector_of(direction)
        image = assemble(operator(jnp.concatenate([vector * first_scale, vector * second_scale], axis=0)))
        alpha = now / total(direction, image)
        trace = trace + alpha * direction
        if step + 1 < CG_STEPS:
            residual = residual - alpha * image
            fresh = total(residual, residual)
            direction = residual + (fresh / now) * direction
            now = fresh
    pieces = parts(trace)
    for i in range(PARTS):
        scr[i, 0:64] = pieces[i]
        scr[i, 64:72] = fold(pieces[i + 1][:32], 0) if i < 3 else jnp.zeros((8, 128), F32)
    for k, ref in enumerate((o0_ref, o1_ref, o2_ref, o3_ref)):
        ref[...] = scr[lax.rem(lax.axis_index("elem") + k, PARTS), 0:72]


def recover_kernel(t0_ref, t1_ref, t2_ref, t3_ref, x_ref, rec_ref, aux_ref, o_ref, scr, t_scr, o_scr, sems):
    for k, ref in enumerate((t0_ref, t1_ref, t2_ref, t3_ref)):
        t_scr[lax.rem(lax.axis_index("elem") + PARTS - k, PARTS), 0:72] = ref[...]
    second = aux_ref[20:21, :]
    p = lanes(32)[0]
    row = lax.broadcasted_iota(jnp.int32, (32, 128), 0)
    vectors = []
    for q in range(4):
        v = t_scr[q, 0:32]
        h = t_scr[q, 32:64]
        right = jnp.where(p < 48, turn(v, -16), unfold(t_scr[q, 64:72], 48))
        vectors.append(jnp.concatenate([v, right, h, jnp.where(row == 31, second, take_top(h))], axis=0))
    turned = jnp.concatenate(vectors, axis=1).T
    kind = turned[:, 127:128]
    recovered = dot3(split(jnp.concatenate([turned * (1.0 - kind), turned * kind], axis=1)), split(rec_ref[...]))
    wave = lax.div(4 * lax.axis_index("planes") + (lax.broadcasted_iota(jnp.int32, (8, 128), 0) & 3) + 1, 2).astype(F32)
    weight = 1.0 / (2.0 + (BETA_COEF * wave) * (BETA_COEF * wave))
    for t in range(2):
        pieces = [recovered[(2 * q + el) * 64:(2 * q + el + 1) * 64, 128 * t:128 * (t + 1)] for el in range(2) for q in range(4)]
        mine = jnp.transpose(jnp.concatenate(pieces, axis=0).reshape(8, GROUPS, 128), (1, 0, 2))
        for g in range(GROUPS):
            scr[512 * t + 8 * g:512 * t + 8 * g + 8, :] = x_ref[16 * g + 8 * t:16 * g + 8 * t + 8, :] * weight + mine[g]
    lane = lax.broadcasted_iota(jnp.int32, (4, 128), 1)

    def leaving(c):
        return pltpu.make_async_copy(o_scr.at[c], o_ref.at[c], sems.at[c])

    for c in range(3):
        current = jnp.zeros((4, 128), F32)
        for e in range(2 * GROUPS):
            tile, offset = divmod(NODE * e, 128)
            rows = jnp.concatenate([scr[4 * e:4 * e + 4, :], scr[512 + 4 * e:516 + 4 * e, :]], axis=1)
            turned = pltpu.roll(rows, (offset - NODE * c) % 256, 1)
            current = jnp.where(lane >= offset, turned[:, :128], current)
            if offset + NODE >= 128:
                o_scr[c, :, 128 * tile:128 * (tile + 1)] = current
                current = turned[:, 128:]
        leaving(c).start()
    for c in range(3):
        leaving(c).wait()


VMEM = pl.BlockSpec(memory_space=pltpu.VMEM)


def shape(*dims):
    return jax.ShapeDtypeStruct(dims, F32)


ANY = pl.BlockSpec(memory_space=pl.ANY)


def call(kernel, name, out, args, scratch=(), sems=(), far_in=False, far_out=False):
    many = isinstance(out, tuple)
    if not far_in:
        args = tuple(pltpu.with_memory_space_constraint(jnp.asarray(a), pltpu.VMEM) for a in args)
    if not far_out:
        outs = tuple(pltpu.VMEM(o.shape, F32) for o in (out if many else (out,)))
        out = outs if many else outs[0]
    place = ANY if far_out else VMEM
    return pl.pallas_call(
        kernel,
        name=name,
        out_shape=out,
        in_specs=[ANY if far_in else VMEM] * len(args),
        out_specs=tuple(place for _ in out) if many else place,
        scratch_shapes=[pltpu.VMEM(dims, F32) for dims in scratch] + [pltpu.SemaphoreType.DMA((n,)) for n in sems],
    )(*args)


def exchange(value, axis, count):
    return lax.all_to_all(value.reshape(count, -1, 128), axis, split_axis=0, concat_axis=0, tiled=True)


def spread(blocks):
    moved = [lax.ppermute(blocks[k], "elem", [(s, (s + k) % PARTS) for s in range(PARTS)]) for k in range(1, PARTS)]
    return (blocks[0],) + tuple(moved)


def per_device(velocity, geometry, element_kind, element_scale, dirichlet, schur_stiffness, schur_mass, lift, recover):
    edge, node, mask_rn, mask_rr, perm, pick = selections()
    packed = call(pack_kernel, "pack", shape(1024, 128), (velocity,),
                  scratch=((3, 4, PART_NODES), (1024, 128)), sems=(PACK_STEPS, PACK_STEPS), far_in=True, far_out=True)
    arrived = exchange(packed, "planes", GROUPS).reshape(1024, 128)
    lift_all, w_all, rec_all, geo, aux = call(
        prep_kernel, "prep",
        (shape(256, 256), shape(128, 256), shape(256, 256), shape(8, 256), shape(24, 128)),
        (geometry, element_kind.reshape(1, 128), element_scale.reshape(1, 128), dirichlet,
         schur_stiffness, schur_mass, lift, recover, edge, node, mask_rn, mask_rr, perm),
        scratch=((24, 128),))
    inter = call(advect_kernel, "advect", shape(1024, 128), (arrived,) + tables() + (geo,),
                 scratch=((512, 256), (512, 256), (256, 256)))
    owned = exchange(inter, "planes", GROUPS).reshape(1024, 128)
    lifted = call(lift_kernel, "lift", (shape(96, 128),) * PARTS, (owned, lift_all, aux),
                  scratch=((512, 256), (PARTS, 96, 128)))
    traces = call(cg_kernel, "cg", (shape(72, 128),) * PARTS, spread(lifted) + (w_all, pick),
                  scratch=((PARTS, 96, 128),))
    return call(recover_kernel, "recover", shape(3, 4, PART_NODES), spread(traces) + (owned, rec_all, aux),
                scratch=((1024, 128), (PARTS, 96, 128), (3, 4, PART_NODES)), sems=(3,), far_out=True)


def solution(mesh):
    in_specs = (
        P(None, "planes", "elem"),
        P(None, "elem"),
        P("elem"),
        P("elem"),
        P(None, None, "elem"),
        P(),
        P(),
        P(),
        P(),
    )
    out_specs = P(None, "planes", "elem")
    return jax.shard_map(per_device, mesh=mesh, in_specs=in_specs, out_specs=out_specs, check_vma=False)
```

```python
import functools

import jax
import jax.numpy as jnp
import ml_dtypes
import numpy as np
from jax import lax
from jax.experimental import pallas as pl
from jax.experimental.pallas import tpu as pltpu
from jax.sharding import PartitionSpec as P

PLANES = 256
QUAD = 9
NODE = QUAD * QUAD
GROUPS = 64
PARTS = 4
PART_NODES = 10368
CG_STEPS = 4
BETA_COEF = 0.01
STEP_DT = 0.002
HIGHEST = lax.Precision.HIGHEST
F32 = jnp.float32
BF16 = jnp.bfloat16


def gauss_derivative(points):
    nodes = -np.cos(np.pi * (2 * np.arange(points) + 1) / (2 * points))
    ident = np.eye(points)
    diffs = nodes[:, None] - nodes[None, :] + ident
    weights = 1.0 / np.prod(diffs, axis=1)
    matrix = (weights[None, :] / weights[:, None]) / diffs
    matrix = matrix * (1.0 - ident)
    return matrix - ident * matrix.sum(axis=1)[:, None]


def split_np(table):
    high = table.astype(np.float32).astype(ml_dtypes.bfloat16)
    low = (table - high.astype(np.float64)).astype(np.float32).astype(ml_dtypes.bfloat16)
    return high, low


@functools.lru_cache(None)
def tables():
    z = np.arange(PLANES)
    rows = np.arange(PLANES)
    waves = (rows + 1) // 2
    angle = 2.0 * np.pi / PLANES * (waves[None, :] * z[:, None] % PLANES)
    cosine, sine = np.cos(angle), np.sin(angle)
    odd = (rows % 2 == 1)[None, :]
    ends = ((rows == 0) | (rows == PLANES - 1))[None, :]
    synth = np.where((rows == 0)[None, :], 1.0, np.where(odd, cosine, sine))
    rate = BETA_COEF * waves[None, :]
    slope = np.where(ends, 0.0, np.where(odd, -rate * sine, rate * cosine))
    weight = np.where(ends[0], 1.0 / PLANES, 2.0 / PLANES)
    analysis = synth.T * weight[:, None]
    deriv = gauss_derivative(QUAD)
    first = np.kron(deriv, np.eye(QUAD))
    second = np.kron(np.eye(QUAD), deriv)
    both = np.zeros((256, 512))
    for c in range(3):
        at = slice(c * NODE, (c + 1) * NODE)
        both[at, c * NODE:(c + 1) * NODE] = first.T
        both[at, 256 + c * NODE:256 + (c + 1) * NODE] = second.T
    out = []
    for table in (np.concatenate([synth, slope], 0), both, analysis):
        out.extend(split_np(table))
    return tuple(out)


@functools.lru_cache(None)
def selections():
    edge = np.zeros((128, 36), np.float32)
    node = np.zeros((256, NODE), np.float32)
    comp_row = np.full(128, -1)
    comp_col = np.full(256, -2)
    for c in range(3):
        for s in range(4):
            for k in range(QUAD):
                edge[s * 32 + c * QUAD + k, s * QUAD + k] = 1
                comp_row[s * 32 + c * QUAD + k] = c
        for n in range(NODE):
            node[c * NODE + n, n] = 1
            comp_col[c * NODE + n] = c
    mask_rn = (comp_row[:, None] == comp_col[None, :]).astype(np.float32)
    mask_rr = ((comp_row[:, None] == comp_row[None, :]) & (comp_row >= 0)[:, None]).astype(np.float32)
    perm = np.zeros((128, 128), np.float32)
    for p in range(GROUPS):
        for el in range(2):
            perm[2 * p + el, el * GROUPS + p] = 1
    pick = np.zeros((64, 24), ml_dtypes.bfloat16)
    for c in range(3):
        for k in range(QUAD):
            pick[c * QUAD + k, 2 + k] = 1
            pick[32 + c * QUAD + k, 11 + k] = 1
    return edge, node, mask_rn, mask_rr, perm, pick


def split(x):
    high = x.astype(BF16)
    return high, (x - high.astype(F32)).astype(BF16)


def dot3(a, b, dims=(((1,), (0,)), ((), ()))):
    mul = functools.partial(lax.dot_general, dimension_numbers=dims, preferred_element_type=F32)
    return mul(a[0], b[0]) + (mul(a[0], b[1]) + mul(a[1], b[0]))


def dot6(a, b, dims=(((1,), (0,)), ((), ()))):
    return lax.dot_general(a, b, dims, precision=HIGHEST, preferred_element_type=F32)


NT = (((1,), (1,)), ((), ()))


PACK_IN = (16, 48, 128)
PACK_OUT = (40, 80, 112, 128)


def window_base(e):
    return min(NODE * e // 128 * 128, PART_NODES - 256)


def pack_kernel(v_ref, o_ref, v_scr, o_scr, in_sems, out_sems):
    lane = lax.broadcasted_iota(jnp.int32, (4, 256), 1)
    col_cuts = [0] + [window_base(e - 1) + 256 for e in PACK_IN]
    row_cuts = [0] + [8 * e for e in PACK_OUT]

    def arriving(g):
        cols = slice(col_cuts[g], col_cuts[g + 1])
        return pltpu.make_async_copy(v_ref.at[:, :, cols], v_scr.at[:, :, cols], in_sems.at[g])

    def leaving(g):
        rows = slice(row_cuts[g], row_cuts[g + 1])
        return pltpu.make_async_copy(o_scr.at[rows], o_ref.at[rows], out_sems.at[g])

    for g in range(len(PACK_IN)):
        arriving(g).start()
    def piece(e, c):
        base = window_base(e)
        return v_scr[c, :, base:base + 128], v_scr[c, :, base + 128:base + 256], (NODE * c - (NODE * e - base)) % 256

    half_row = lax.broadcasted_iota(jnp.int32, (8, 256), 0) >> 2
    both_lane = lax.broadcasted_iota(jnp.int32, (8, 256), 1) - NODE * half_row
    for e in range(0, 2 * GROUPS, 2):
        if e in (0,) + PACK_IN[:-1]:
            arriving(((0,) + PACK_IN).index(e)).wait()
        rows = jnp.zeros((8, 256), F32)
        for c in range(2):
            low, high, shift = piece(e, c)
            other = piece(e + 1, c + 1)
            swap = (other[2] - shift) % 256 != 0
            window = jnp.concatenate([jnp.concatenate([low, other[int(swap)]], axis=0),
                                      jnp.concatenate([high, other[1 - int(swap)]], axis=0)], axis=1)
            rows = jnp.where((both_lane >= NODE * c) & (both_lane < NODE * (c + 1)), pltpu.roll(window, shift, 1), rows)
        low, high, shift = piece(e, 2)
        third = pltpu.roll(jnp.concatenate([low, high], axis=1), shift, 1)
        low, high, shift = piece(e + 1, 0)
        first = pltpu.roll(jnp.concatenate([low, high], axis=1), shift, 1)
        rest = jnp.concatenate([jnp.where(lane < 3 * NODE, x, 0.0) for x in (third, first)], axis=0)
        rows = jnp.where((both_lane >= 2 * NODE) | (both_lane < 0), rest, rows)
        o_scr[8 * e:8 * e + 8, :] = rows[:, :128]
        o_scr[8 * e + 8:8 * e + 16, :] = rows[:, 128:]
        if e + 2 in PACK_OUT:
            leaving(PACK_OUT.index(e + 2)).start()
    for g in range(len(PACK_OUT)):
        leaving(g).wait()


def prep_kernel(geo_ref, kind_ref, scale_ref, dir_ref, stiff_ref, mass_ref, lift_ref, rec_ref,
                edge_ref, node_ref, mrn_ref, mrr_ref, perm_ref,
                lift_high, lift_low, w_out, rec_high, rec_low, geo_out, aux_out, aux_scr):
    place = lax.axis_index("planes")
    lane = lax.broadcasted_iota(jnp.int32, (4, 256), 1)
    for el in range(2):
        start = 2 * NODE * place + NODE * el
        base = pl.multiple_of(jnp.minimum(lax.div(start, 128) * 128, PART_NODES - 256), 128)
        window = geo_ref[:, pl.ds(base, 256)]
        turned = pltpu.roll(window, lax.rem(256 - (start - base), 256), 1)
        tiled = jnp.where(lane < NODE, turned,
                          jnp.where(lane < 2 * NODE, pltpu.roll(turned, NODE, 1), pltpu.roll(turned, 2 * NODE, 1)))
        geo_out[4 * el:4 * el + 4, :] = jnp.where(lane < 3 * NODE, tiled, 0.0)
    wave = lax.div(4 * place + lax.axis_index("elem") + 1, 2).astype(F32)
    lam = 1.0 + (BETA_COEF * wave) * (BETA_COEF * wave)
    edge = edge_ref[...]
    node = node_ref[...]
    for t in range(2):
        rows = slice(128 * t, 128 * (t + 1))
        lift_high[rows, :], lift_low[rows, :] = split(dot6(dot6(edge, lift_ref[t]), node, NT) * mrn_ref[...])
        rec_high[rows, :], rec_low[rows, :] = split(dot6(dot6(edge, rec_ref[t], NT), node, NT) * mrn_ref[...])
        mixed = stiff_ref[t] + lam * mass_ref[t]
        w_out[:128, rows], w_out[128:, rows] = split(dot6(dot6(edge, mixed), edge, NT) * mrr_ref[...])
    second = (kind_ref[...] == 1).astype(F32)
    aux_scr[...] = jnp.zeros((24, 128), F32)
    aux_scr[0:1, :] = scale_ref[...] * (1.0 - second)
    aux_scr[1:2, :] = scale_ref[...] * second
    aux_scr[2:11, :] = (1 - dir_ref[0]).astype(F32)
    aux_scr[11:20, :] = (1 - dir_ref[1]).astype(F32)
    aux_scr[20:21, :] = second
    aux_out[...] = dot6(aux_scr[...], perm_ref[...])


def swap_halves(x, y):
    first = lax.broadcasted_iota(jnp.int32, x.shape, 1) < 4
    return jnp.where(first, x, pltpu.roll(y, 4, 1)), jnp.where(first, pltpu.roll(x, 4, 1), y)


def advect_kernel(x_ref, th_ref, tl_ref, dh_ref, dl_ref, ah_ref, al_ref, geo_ref, o_ref, items_scr, synth_scr, adv_scr):
    lane = lax.broadcasted_iota(jnp.int32, (256, 256), 1)
    low = lane < NODE
    mid = lane < 2 * NODE
    for t in range(2):
        pairs = [jnp.concatenate([x_ref[32 * m + 16 * odd + 8 * t:32 * m + 16 * odd + 8 * t + 8, :] for m in range(32)], axis=0)
                 .reshape(32, 8, 128) for odd in range(2)]
        for el, rows in enumerate(swap_halves(*pairs)):
            items_scr[256 * el:256 * (el + 1), 128 * t:128 * (t + 1)] = rows.reshape(256, 128)
    for el in range(2):
        here = slice(256 * el, 256 * (el + 1))
        synth_scr[...] = dot3((th_ref[...], tl_ref[...]), split(items_scr[here, :]))
        geo = geo_ref[4 * el:4 * el + 4, :]
        values = synth_scr[:256, :]
        both = dot3(split(values), (dh_ref[...], dl_ref[...]))
        along_r = both[:, :256]
        along_s = both[:, 256:]
        along_x = geo[0:1] * along_r + geo[1:2] * along_s
        along_y = geo[2:3] * along_r + geo[3:4] * along_s
        up = pltpu.roll(values, NODE, 1)
        up2 = pltpu.roll(values, 2 * NODE, 1)
        down = pltpu.roll(values, 256 - NODE, 1)
        down2 = pltpu.roll(values, 256 - 2 * NODE, 1)
        u = jnp.where(low, values, jnp.where(mid, up, up2))
        v = jnp.where(low, down, jnp.where(mid, values, up))
        w = jnp.where(low, down2, jnp.where(mid, down, values))
        adv_scr[...] = u * along_x + v * along_y + w * synth_scr[256:, :]
        hat = dot3((ah_ref[...], al_ref[...]), split(adv_scr[...]))
        items_scr[here, :] = items_scr[here, :] - STEP_DT * hat
    for t in range(2):
        elems = [items_scr[256 * el:256 * (el + 1), 128 * t:128 * (t + 1)].reshape(32, 8, 128) for el in range(2)]
        for odd, rows in enumerate(swap_halves(*elems)):
            for m in range(32):
                at = 32 * m + 16 * odd + 8 * t
                o_ref[at:at + 8, :] = rows[m]


def turn(x, shift):
    return pltpu.roll(x, shift % 128, 1)


def lanes(rows):
    lane = lax.broadcasted_iota(jnp.int32, (rows, 128), 1)
    p = lane & 63
    el = lane >> 6
    return p, el, 2 * (p & 15) + el


def fold(x, first):
    group = lanes(8)[0] >> 4
    out = jnp.zeros((8, 128), F32)
    for g in range(4):
        out = jnp.where(group == g, turn(x[8 * g:8 * g + 8], 16 * g - first), out)
    return out


def unfold(x, first):
    return jnp.concatenate([turn(x, first - 16 * g) for g in range(4)], axis=0)


def put_halo(ref, x):
    ref[27:32] = x[0:5]
    ref[59:62] = x[5:8]


def get_halo(ref, scr):
    scr[0:5] = ref[27:32]
    scr[5:8] = ref[59:62]
    return scr[...]


def take_top(h):
    p, el, height = lanes(32)
    return jnp.where(height == 31, 0.0, jnp.where(el == 0, turn(h, 64), turn(h, 63)))


def give_top(h):
    p, el, height = lanes(32)
    return jnp.where(height == 0, 0.0, jnp.where(el == 1, turn(h, 64), turn(h, -63)))


def lift_kernel(x_ref, lift_high, lift_low, aux_ref, o0_ref, o1_ref, o2_ref, o3_ref, in_scr, out_scr):
    arrived = jnp.transpose(x_ref[...].reshape(GROUPS, 16, 128), (1, 0, 2))
    for q in range(4):
        for el in range(2):
            at = (2 * q + el) * 64
            for t in range(2):
                in_scr[at:at + 64, t * 128:(t + 1) * 128] = arrived[t * 8 + el * 4 + q]
    lifted = dot3((lift_high[...], lift_low[...]), split(in_scr[...]), NT)
    second = aux_ref[20:21, :] > 0.5
    p = lanes(32)[0]
    for q in range(4):
        cols = slice(128 * q, 128 * (q + 1))
        edges = jnp.where(second, lifted[128:, cols], lifted[:128, cols])
        right = edges[32:64]
        out_scr[q, 0:32] = edges[0:32] + jnp.where(p >= 16, turn(right, 16), 0.0)
        out_scr[q, 32:64] = edges[64:96] + give_top(edges[96:128])
        put_halo(out_scr.at[q], fold(right, 48))
        out_scr[q, 64:88] = aux_ref[...]
    for k, ref in enumerate((o0_ref, o1_ref, o2_ref, o3_ref)):
        ref[...] = out_scr[lax.rem(lax.axis_index("elem") + k, PARTS)]


def cg_kernel(f0_ref, f1_ref, f2_ref, f3_ref, w_ref, pick_ref, o0_ref, o1_ref, o2_ref, o3_ref, scr, halo_scr):
    for k, ref in enumerate((f0_ref, f1_ref, f2_ref, f3_ref)):
        scr[lax.rem(lax.axis_index("elem") + PARTS - k, PARTS)] = ref[...]
    p = lanes(32)[0]
    sub = lax.broadcasted_iota(jnp.int32, (64, 1), 0) & 31
    comp = (sub >= QUAD).astype(jnp.int32) + (sub >= 2 * QUAD).astype(jnp.int32)
    zero = jnp.zeros((32, 128), F32)

    def parts(x):
        return [x[:, 128 * i:128 * (i + 1)] for i in range(PARTS)]

    def right_of(v):
        v = parts(v)
        return jnp.concatenate([jnp.where(p < 48, turn(v[i], -16), turn(v[i + 1], 48) if i < 3 else zero)
                                for i in range(PARTS)], axis=1)

    def from_left(v):
        v = parts(v)
        return jnp.concatenate([jnp.where(p >= 16, turn(v[i], 16), turn(v[i - 1], -48) if i > 0 else zero)
                                for i in range(PARTS)], axis=1)

    def top_of(h):
        return jnp.concatenate([take_top(x) for x in parts(h)], axis=1)

    def from_below(h):
        return jnp.concatenate([give_top(x) for x in parts(h)], axis=1)

    def vector_of(x):
        v, h = x[:32], x[32:]
        return jnp.concatenate([v, right_of(v), h, top_of(h)], axis=0)

    aux = jnp.concatenate([scr[i, 64:88] for i in range(PARTS)], axis=1)
    free = lax.dot(pick_ref[...], aux.astype(BF16), preferred_element_type=F32)
    first_scale = aux[0:1]
    second_scale = aux[1:2]
    w_both = w_ref[...]
    w_high = w_both[:128]

    def operator(x):
        high, low = split(x)
        both = lax.dot(w_both, high, preferred_element_type=F32)
        return both[:128] + (both[128:] + lax.dot(w_high, low, preferred_element_type=F32))

    def assemble(y):
        return jnp.concatenate([y[:32] + from_left(y[32:64]), y[64:96] + from_below(y[96:])], axis=0) * free

    def total(a, b):
        line = jnp.sum(a * b, axis=1, keepdims=True)
        sums = [jnp.sum(jnp.where(comp == c, line, 0.0), axis=0, keepdims=True) for c in range(3)]
        return jnp.where(comp == 0, sums[0], jnp.where(comp == 1, sums[1], sums[2]))

    sent = []
    for i in range(PARTS):
        v = scr[i, 0:32]
        if i > 0:
            v = v + jnp.where(p < 16, unfold(get_halo(scr.at[i - 1], halo_scr.at[i - 1]), 0), 0.0)
        sent.append(jnp.concatenate([v, scr[i, 32:64]], axis=0))
    residual = jnp.concatenate(sent, axis=1) * free
    direction = residual
    trace = jnp.zeros_like(residual)
    now = total(residual, residual)
    for step in range(CG_STEPS):
        vector = vector_of(direction)
        image = assemble(operator(jnp.concatenate([vector * first_scale, vector * second_scale], axis=0)))
        alpha = now / total(direction, image)
        trace = trace + alpha * direction
        if step + 1 < CG_STEPS:
            residual = residual - alpha * image
            fresh = total(residual, residual)
            direction = residual + (fresh / now) * direction
            now = fresh
    pieces = parts(trace)
    for i in range(PARTS):
        scr[i, 0:64] = pieces[i]
        put_halo(scr.at[i], fold(pieces[i + 1][:32], 0) if i < 3 else jnp.zeros((8, 128), F32))
    for k, ref in enumerate((o0_ref, o1_ref, o2_ref, o3_ref)):
        ref[...] = scr[lax.rem(lax.axis_index("elem") + k, PARTS), 0:64]


def recover_kernel(t0_ref, t1_ref, t2_ref, t3_ref, x_ref, rec_high, rec_low, aux_ref, o_ref, scr, t_scr, o_scr, halo_scr, sems):
    for k, ref in enumerate((t0_ref, t1_ref, t2_ref, t3_ref)):
        t_scr[lax.rem(lax.axis_index("elem") + PARTS - k, PARTS), 0:64] = ref[...]
    second = aux_ref[20:21, :]
    p = lanes(32)[0]
    row = lax.broadcasted_iota(jnp.int32, (32, 128), 0)
    vectors = []
    for q in range(4):
        v = t_scr[q, 0:32]
        h = t_scr[q, 32:64]
        right = jnp.where(p < 48, turn(v, -16), unfold(get_halo(t_scr.at[q], halo_scr.at[q]), 48))
        vectors.append(jnp.concatenate([v, right, h, jnp.where(row == 31, second, take_top(h))], axis=0))
    turned = jnp.concatenate(vectors, axis=1).T
    kind = turned[:, 127:128]
    recovered = dot3(split(jnp.concatenate([turned * (1.0 - kind), turned * kind], axis=1)), (rec_high[...], rec_low[...]))
    wave = lax.div(4 * lax.axis_index("planes") + (lax.broadcasted_iota(jnp.int32, (8, 128), 0) & 3) + 1, 2).astype(F32)
    weight = 1.0 / (2.0 + (BETA_COEF * wave) * (BETA_COEF * wave))
    for t in range(2):
        pieces = [recovered[(2 * q + el) * 64:(2 * q + el + 1) * 64, 128 * t:128 * (t + 1)] for el in range(2) for q in range(4)]
        mine = jnp.transpose(jnp.concatenate(pieces, axis=0).reshape(8, GROUPS, 128), (1, 0, 2))
        for g in range(GROUPS):
            scr[512 * t + 8 * g:512 * t + 8 * g + 8, :] = x_ref[16 * g + 8 * t:16 * g + 8 * t + 8, :] * weight + mine[g]
    lane = lax.broadcasted_iota(jnp.int32, (4, 128), 1)

    cuts = (0, 5376, PART_NODES)

    def leaving(c, part):
        cols = slice(cuts[part], cuts[part + 1])
        return pltpu.make_async_copy(o_scr.at[c, :, cols], o_ref.at[c, :, cols], sems.at[2 * c + part])

    for c in range(3):
        current = jnp.zeros((4, 128), F32)
        for e in range(2 * GROUPS):
            tile, offset = divmod(NODE * e, 128)
            rows = jnp.concatenate([scr[4 * e:4 * e + 4, :], scr[512 + 4 * e:516 + 4 * e, :]], axis=1)
            turned = pltpu.roll(rows, (offset - NODE * c) % 256, 1)
            current = jnp.where(lane >= offset, turned[:, :128], current)
            if offset + NODE >= 128:
                o_scr[c, :, 128 * tile:128 * (tile + 1)] = current
                current = turned[:, 128:]
                if 128 * (tile + 1) in cuts:
                    leaving(c, cuts.index(128 * (tile + 1)) - 1).start()
    for c in range(3):
        for part in range(2):
            leaving(c, part).wait()


VMEM = pl.BlockSpec(memory_space=pltpu.VMEM)


def shape(*dims):
    return jax.ShapeDtypeStruct(dims, F32)


ANY = pl.BlockSpec(memory_space=pl.ANY)


def half(*dims):
    return jax.ShapeDtypeStruct(dims, BF16)


def call(kernel, name, out, args, scratch=(), sems=(), far_in=False, far_out=False):
    many = isinstance(out, tuple)
    if not far_in:
        args = tuple(pltpu.with_memory_space_constraint(jnp.asarray(a), pltpu.VMEM) for a in args)
    if not far_out:
        outs = tuple(pltpu.VMEM(o.shape, o.dtype) for o in (out if many else (out,)))
        out = outs if many else outs[0]
    place = ANY if far_out else VMEM
    return pl.pallas_call(
        kernel,
        name=name,
        out_shape=out,
        in_specs=[ANY if far_in else VMEM] * len(args),
        out_specs=tuple(place for _ in out) if many else place,
        scratch_shapes=[pltpu.VMEM(dims, F32) for dims in scratch] + [pltpu.SemaphoreType.DMA((n,)) for n in sems],
    )(*args)


def exchange(value, axis, count):
    return lax.all_to_all(value.reshape(count, -1, 128), axis, split_axis=0, concat_axis=0, tiled=True)


def spread(blocks):
    moved = [lax.ppermute(blocks[k], "elem", [(s, (s + k) % PARTS) for s in range(PARTS)]) for k in range(1, PARTS)]
    return (blocks[0],) + tuple(moved)


def per_device(velocity, geometry, element_kind, element_scale, dirichlet, schur_stiffness, schur_mass, lift, recover):
    edge, node, mask_rn, mask_rr, perm, pick = selections()
    packed = call(pack_kernel, "pack", shape(1024, 128), (velocity,),
                  scratch=((3, 4, PART_NODES), (1024, 128)), sems=(len(PACK_IN), len(PACK_OUT)), far_in=True, far_out=True)
    arrived = exchange(packed, "planes", GROUPS).reshape(1024, 128)
    lift_high, lift_low, w_all, rec_high, rec_low, geo, aux = call(
        prep_kernel, "prep",
        (half(256, 256), half(256, 256), half(256, 256), half(256, 256), half(256, 256), shape(8, 256), shape(24, 128)),
        (geometry, element_kind.reshape(1, 128), element_scale.reshape(1, 128), dirichlet,
         schur_stiffness, schur_mass, lift, recover, edge, node, mask_rn, mask_rr, perm),
        scratch=((24, 128),))
    inter = call(advect_kernel, "advect", shape(1024, 128), (arrived,) + tables() + (geo,),
                 scratch=((512, 256), (512, 256), (256, 256)))
    owned = exchange(inter, "planes", GROUPS).reshape(1024, 128)
    lifted = call(lift_kernel, "lift", (shape(88, 128),) * PARTS, (owned, lift_high, lift_low, aux),
                  scratch=((512, 256), (PARTS, 88, 128)))
    traces = call(cg_kernel, "cg", (shape(64, 128),) * PARTS, spread(lifted) + (w_all, pick),
                  scratch=((PARTS, 88, 128), (PARTS, 8, 128)))
    return call(recover_kernel, "recover", shape(3, 4, PART_NODES), spread(traces) + (owned, rec_high, rec_low, aux),
                scratch=((1024, 128), (PARTS, 88, 128), (3, 4, PART_NODES), (PARTS, 8, 128)), sems=(6,), far_out=True)


def solution(mesh):
    in_specs = (
        P(None, "planes", "elem"),
        P(None, "elem"),
        P("elem"),
        P("elem"),
        P(None, None, "elem"),
        P(),
        P(),
        P(),
        P(),
    )
    out_specs = P(None, "planes", "elem")
    return jax.shard_map(per_device, mesh=mesh, in_specs=in_specs, out_specs=out_specs, check_vma=False)
```

```python
import functools

import jax
import jax.numpy as jnp
import ml_dtypes
import numpy as np
from jax import lax
from jax.experimental import pallas as pl
from jax.experimental.pallas import tpu as pltpu
from jax.sharding import PartitionSpec as P

PLANES = 256
QUAD = 9
NODE = QUAD * QUAD
GROUPS = 64
PARTS = 4
PART_NODES = 10368
CG_STEPS = 4
BETA_COEF = 0.01
STEP_DT = 0.002
HIGHEST = lax.Precision.HIGHEST
F32 = jnp.float32
BF16 = jnp.bfloat16


def gauss_derivative(points):
    nodes = -np.cos(np.pi * (2 * np.arange(points) + 1) / (2 * points))
    ident = np.eye(points)
    diffs = nodes[:, None] - nodes[None, :] + ident
    weights = 1.0 / np.prod(diffs, axis=1)
    matrix = (weights[None, :] / weights[:, None]) / diffs
    matrix = matrix * (1.0 - ident)
    return matrix - ident * matrix.sum(axis=1)[:, None]


def split_np(table):
    high = table.astype(np.float32).astype(ml_dtypes.bfloat16)
    low = (table - high.astype(np.float64)).astype(np.float32).astype(ml_dtypes.bfloat16)
    return high, low


@functools.lru_cache(None)
def tables():
    z = np.arange(PLANES)
    rows = np.arange(PLANES)
    waves = (rows + 1) // 2
    angle = 2.0 * np.pi / PLANES * (waves[None, :] * z[:, None] % PLANES)
    cosine, sine = np.cos(angle), np.sin(angle)
    odd = (rows % 2 == 1)[None, :]
    ends = ((rows == 0) | (rows == PLANES - 1))[None, :]
    synth = np.where((rows == 0)[None, :], 1.0, np.where(odd, cosine, sine))
    rate = BETA_COEF * waves[None, :]
    slope = np.where(ends, 0.0, np.where(odd, -rate * sine, rate * cosine))
    weight = np.where(ends[0], 1.0 / PLANES, 2.0 / PLANES)
    analysis = synth.T * weight[:, None]
    deriv = gauss_derivative(QUAD)
    first = np.kron(deriv, np.eye(QUAD))
    second = np.kron(np.eye(QUAD), deriv)
    both = np.zeros((256, 512))
    for c in range(3):
        at = slice(c * NODE, (c + 1) * NODE)
        both[at, c * NODE:(c + 1) * NODE] = first.T
        both[at, 256 + c * NODE:256 + (c + 1) * NODE] = second.T
    out = []
    for table in (np.concatenate([synth, slope], 0), both, analysis):
        out.extend(split_np(table))
    return tuple(out)


@functools.lru_cache(None)
def selections():
    edge = np.zeros((128, 36), np.float32)
    node = np.zeros((256, NODE), np.float32)
    comp_row = np.full(128, -1)
    comp_col = np.full(256, -2)
    for c in range(3):
        for s in range(4):
            for k in range(QUAD):
                edge[s * 32 + c * QUAD + k, s * QUAD + k] = 1
                comp_row[s * 32 + c * QUAD + k] = c
        for n in range(NODE):
            node[c * NODE + n, n] = 1
            comp_col[c * NODE + n] = c
    mask_rn = (comp_row[:, None] == comp_col[None, :]).astype(np.float32)
    mask_rr = ((comp_row[:, None] == comp_row[None, :]) & (comp_row >= 0)[:, None]).astype(np.float32)
    perm = np.zeros((128, 128), np.float32)
    for p in range(GROUPS):
        for el in range(2):
            perm[2 * p + el, el * GROUPS + p] = 1
    pick = np.zeros((64, 24), ml_dtypes.bfloat16)
    for c in range(3):
        for k in range(QUAD):
            pick[c * QUAD + k, 2 + k] = 1
            pick[32 + c * QUAD + k, 11 + k] = 1
    return edge, node, mask_rn, mask_rr, perm, pick


def split(x):
    high = x.astype(BF16)
    return high, (x - high.astype(F32)).astype(BF16)


def dot3(a, b, dims=(((1,), (0,)), ((), ()))):
    mul = functools.partial(lax.dot_general, dimension_numbers=dims, preferred_element_type=F32)
    return mul(a[0], b[0]) + (mul(a[0], b[1]) + mul(a[1], b[0]))


def dot6(a, b, dims=(((1,), (0,)), ((), ()))):
    return lax.dot_general(a, b, dims, precision=HIGHEST, preferred_element_type=F32)


NT = (((1,), (1,)), ((), ()))


PACK_IN = (16, 48, 128)
PACK_OUT = (48, 96, 120, 128)


def window_base(e):
    return min(NODE * e // 128 * 128, PART_NODES - 256)


def pack_kernel(v_ref, o_ref, v_scr, o_scr, in_sems, out_sems):
    lane = lax.broadcasted_iota(jnp.int32, (4, 256), 1)
    col_cuts = [0] + [window_base(e - 1) + 256 for e in PACK_IN]
    row_cuts = [0] + [8 * e for e in PACK_OUT]

    def arriving(g):
        cols = slice(col_cuts[g], col_cuts[g + 1])
        return pltpu.make_async_copy(v_ref.at[:, :, cols], v_scr.at[:, :, cols], in_sems.at[g])

    def leaving(g):
        rows = slice(row_cuts[g], row_cuts[g + 1])
        return pltpu.make_async_copy(o_scr.at[rows], o_ref.at[rows], out_sems.at[g])

    for g in range(len(PACK_IN)):
        arriving(g).start()
    def piece(e, c):
        base = window_base(e)
        return v_scr[c, :, base:base + 128], v_scr[c, :, base + 128:base + 256], (NODE * c - (NODE * e - base)) % 256

    half_row = lax.broadcasted_iota(jnp.int32, (8, 256), 0) >> 2
    both_lane = lax.broadcasted_iota(jnp.int32, (8, 256), 1) - NODE * half_row
    for e in range(0, 2 * GROUPS, 2):
        if e in (0,) + PACK_IN[:-1]:
            arriving(((0,) + PACK_IN).index(e)).wait()
        rows = jnp.zeros((8, 256), F32)
        for c in range(2):
            low, high, shift = piece(e, c)
            other = piece(e + 1, c + 1)
            swap = (other[2] - shift) % 256 != 0
            window = jnp.concatenate([jnp.concatenate([low, other[int(swap)]], axis=0),
                                      jnp.concatenate([high, other[1 - int(swap)]], axis=0)], axis=1)
            rows = jnp.where((both_lane >= NODE * c) & (both_lane < NODE * (c + 1)), pltpu.roll(window, shift, 1), rows)
        low, high, shift = piece(e, 2)
        third = pltpu.roll(jnp.concatenate([low, high], axis=1), shift, 1)
        low, high, shift = piece(e + 1, 0)
        first = pltpu.roll(jnp.concatenate([low, high], axis=1), shift, 1)
        rest = jnp.concatenate([jnp.where(lane < 3 * NODE, x, 0.0) for x in (third, first)], axis=0)
        rows = jnp.where((both_lane >= 2 * NODE) | (both_lane < 0), rest, rows)
        o_scr[8 * e:8 * e + 8, :] = rows[:, :128]
        o_scr[8 * e + 8:8 * e + 16, :] = rows[:, 128:]
        if e + 2 in PACK_OUT:
            leaving(PACK_OUT.index(e + 2)).start()
    for g in range(len(PACK_OUT)):
        leaving(g).wait()


def prep_kernel(geo_ref, kind_ref, scale_ref, dir_ref, stiff_ref, mass_ref, lift_ref, rec_ref,
                edge_ref, node_ref, mrn_ref, mrr_ref, perm_ref,
                lift_high, lift_low, w_out, rec_high, rec_low, geo_out, aux_out, aux_scr):
    place = lax.axis_index("planes")
    lane = lax.broadcasted_iota(jnp.int32, (4, 256), 1)
    for el in range(2):
        start = 2 * NODE * place + NODE * el
        base = pl.multiple_of(jnp.minimum(lax.div(start, 128) * 128, PART_NODES - 256), 128)
        window = geo_ref[:, pl.ds(base, 256)]
        turned = pltpu.roll(window, lax.rem(256 - (start - base), 256), 1)
        tiled = jnp.where(lane < NODE, turned,
                          jnp.where(lane < 2 * NODE, pltpu.roll(turned, NODE, 1), pltpu.roll(turned, 2 * NODE, 1)))
        geo_out[4 * el:4 * el + 4, :] = jnp.where(lane < 3 * NODE, tiled, 0.0)
    wave = lax.div(4 * place + lax.axis_index("elem") + 1, 2).astype(F32)
    lam = 1.0 + (BETA_COEF * wave) * (BETA_COEF * wave)
    edge = edge_ref[...]
    node = node_ref[...]
    for t in range(2):
        rows = slice(128 * t, 128 * (t + 1))
        lift_high[rows, :], lift_low[rows, :] = split(dot6(dot6(edge, lift_ref[t]), node, NT) * mrn_ref[...])
        rec_high[rows, :], rec_low[rows, :] = split(dot6(dot6(edge, rec_ref[t], NT), node, NT) * mrn_ref[...])
        mixed = stiff_ref[t] + lam * mass_ref[t]
        w_out[:128, rows], w_out[128:, rows] = split(dot6(dot6(edge, mixed), edge, NT) * mrr_ref[...])
    second = (kind_ref[...] == 1).astype(F32)
    aux_scr[...] = jnp.zeros((24, 128), F32)
    aux_scr[0:1, :] = scale_ref[...] * (1.0 - second)
    aux_scr[1:2, :] = scale_ref[...] * second
    aux_scr[2:11, :] = (1 - dir_ref[0]).astype(F32)
    aux_scr[11:20, :] = (1 - dir_ref[1]).astype(F32)
    aux_scr[20:21, :] = second
    aux_out[...] = dot6(aux_scr[...], perm_ref[...])


def swap_halves(x, y):
    first = lax.broadcasted_iota(jnp.int32, x.shape, 1) < 4
    return jnp.where(first, x, pltpu.roll(y, 4, 1)), jnp.where(first, pltpu.roll(x, 4, 1), y)


def advect_kernel(x_ref, th_ref, tl_ref, dh_ref, dl_ref, ah_ref, al_ref, geo_ref, o_ref, items_scr, synth_scr, adv_scr):
    lane = lax.broadcasted_iota(jnp.int32, (256, 256), 1)
    low = lane < NODE
    mid = lane < 2 * NODE
    for t in range(2):
        pairs = [jnp.concatenate([x_ref[32 * m + 16 * odd + 8 * t:32 * m + 16 * odd + 8 * t + 8, :] for m in range(32)], axis=0)
                 .reshape(32, 8, 128) for odd in range(2)]
        for el, rows in enumerate(swap_halves(*pairs)):
            items_scr[256 * el:256 * (el + 1), 128 * t:128 * (t + 1)] = rows.reshape(256, 128)
    for el in range(2):
        here = slice(256 * el, 256 * (el + 1))
        synth_scr[...] = dot3((th_ref[...], tl_ref[...]), split(items_scr[here, :]))
        geo = geo_ref[4 * el:4 * el + 4, :]
        values = synth_scr[:256, :]
        both = dot3(split(values), (dh_ref[...], dl_ref[...]))
        along_r = both[:, :256]
        along_s = both[:, 256:]
        along_x = geo[0:1] * along_r + geo[1:2] * along_s
        along_y = geo[2:3] * along_r + geo[3:4] * along_s
        up = pltpu.roll(values, NODE, 1)
        up2 = pltpu.roll(values, 2 * NODE, 1)
        down = pltpu.roll(values, 256 - NODE, 1)
        down2 = pltpu.roll(values, 256 - 2 * NODE, 1)
        u = jnp.where(low, values, jnp.where(mid, up, up2))
        v = jnp.where(low, down, jnp.where(mid, values, up))
        w = jnp.where(low, down2, jnp.where(mid, down, values))
        adv_scr[...] = u * along_x + v * along_y + w * synth_scr[256:, :]
        hat = dot3((ah_ref[...], al_ref[...]), split(adv_scr[...]))
        items_scr[here, :] = items_scr[here, :] - STEP_DT * hat
    for t in range(2):
        elems = [items_scr[256 * el:256 * (el + 1), 128 * t:128 * (t + 1)].reshape(32, 8, 128) for el in range(2)]
        for odd, rows in enumerate(swap_halves(*elems)):
            for m in range(32):
                at = 32 * m + 16 * odd + 8 * t
                o_ref[at:at + 8, :] = rows[m]


def turn(x, shift):
    return pltpu.roll(x, shift % 128, 1)


def lanes(rows):
    lane = lax.broadcasted_iota(jnp.int32, (rows, 128), 1)
    p = lane & 63
    el = lane >> 6
    return p, el, 2 * (p & 15) + el


def fold(x, first):
    group = lanes(8)[0] >> 4
    out = jnp.zeros((8, 128), F32)
    for g in range(4):
        out = jnp.where(group == g, turn(x[8 * g:8 * g + 8], 16 * g - first), out)
    return out


def unfold(x, first):
    return jnp.concatenate([turn(x, first - 16 * g) for g in range(4)], axis=0)


def put_halo(ref, x):
    ref[27:32] = x[0:5]
    ref[59:62] = x[5:8]


def get_halo(ref, scr):
    scr[0:5] = ref[27:32]
    scr[5:8] = ref[59:62]
    return scr[...]


def take_top(h):
    p, el, height = lanes(32)
    return jnp.where(height == 31, 0.0, jnp.where(el == 0, turn(h, 64), turn(h, 63)))


def give_top(h):
    p, el, height = lanes(32)
    return jnp.where(height == 0, 0.0, jnp.where(el == 1, turn(h, 64), turn(h, -63)))


def lift_kernel(x_ref, lift_high, lift_low, aux_ref, o0_ref, o1_ref, o2_ref, o3_ref, in_scr, out_scr):
    arrived = jnp.transpose(x_ref[...].reshape(GROUPS, 16, 128), (1, 0, 2))
    for q in range(4):
        for el in range(2):
            at = (2 * q + el) * 64
            for t in range(2):
                in_scr[at:at + 64, t * 128:(t + 1) * 128] = arrived[t * 8 + el * 4 + q]
    lifted = dot3((lift_high[...], lift_low[...]), split(in_scr[...]), NT)
    second = aux_ref[20:21, :] > 0.5
    p = lanes(32)[0]
    for q in range(4):
        cols = slice(128 * q, 128 * (q + 1))
        edges = jnp.where(second, lifted[128:, cols], lifted[:128, cols])
        right = edges[32:64]
        out_scr[q, 0:32] = edges[0:32] + jnp.where(p >= 16, turn(right, 16), 0.0)
        out_scr[q, 32:64] = edges[64:96] + give_top(edges[96:128])
        put_halo(out_scr.at[q], fold(right, 48))
        out_scr[q, 64:88] = aux_ref[...]
    for k, ref in enumerate((o0_ref, o1_ref, o2_ref, o3_ref)):
        ref[...] = out_scr[lax.rem(lax.axis_index("elem") + k, PARTS)]


def cg_kernel(f0_ref, f1_ref, f2_ref, f3_ref, w_ref, pick_ref, o0_ref, o1_ref, o2_ref, o3_ref, scr, halo_scr):
    for k, ref in enumerate((f0_ref, f1_ref, f2_ref, f3_ref)):
        scr[lax.rem(lax.axis_index("elem") + PARTS - k, PARTS)] = ref[...]
    p = lanes(32)[0]
    sub = lax.broadcasted_iota(jnp.int32, (64, 1), 0) & 31
    comp = (sub >= QUAD).astype(jnp.int32) + (sub >= 2 * QUAD).astype(jnp.int32)
    zero = jnp.zeros((32, 128), F32)

    def parts(x):
        return [x[:, 128 * i:128 * (i + 1)] for i in range(PARTS)]

    def right_of(v):
        v = parts(v)
        return jnp.concatenate([jnp.where(p < 48, turn(v[i], -16), turn(v[i + 1], 48) if i < 3 else zero)
                                for i in range(PARTS)], axis=1)

    def from_left(v):
        v = parts(v)
        return jnp.concatenate([jnp.where(p >= 16, turn(v[i], 16), turn(v[i - 1], -48) if i > 0 else zero)
                                for i in range(PARTS)], axis=1)

    def top_of(h):
        return jnp.concatenate([take_top(x) for x in parts(h)], axis=1)

    def from_below(h):
        return jnp.concatenate([give_top(x) for x in parts(h)], axis=1)

    def vector_of(x):
        v, h = x[:32], x[32:]
        return jnp.concatenate([v, right_of(v), h, top_of(h)], axis=0)

    aux = jnp.concatenate([scr[i, 64:88] for i in range(PARTS)], axis=1)
    free = lax.dot(pick_ref[...], aux.astype(BF16), preferred_element_type=F32)
    first_scale = aux[0:1]
    second_scale = aux[1:2]
    w_both = w_ref[...]
    w_high = w_both[:128]

    def operator(x):
        high, low = split(x)
        both = lax.dot(w_both, high, preferred_element_type=F32)
        return both[:128] + (both[128:] + lax.dot(w_high, low, preferred_element_type=F32))

    def assemble(y):
        return jnp.concatenate([y[:32] + from_left(y[32:64]), y[64:96] + from_below(y[96:])], axis=0) * free

    def total(a, b):
        line = jnp.sum(a * b, axis=1, keepdims=True)
        sums = [jnp.sum(jnp.where(comp == c, line, 0.0), axis=0, keepdims=True) for c in range(3)]
        return jnp.where(comp == 0, sums[0], jnp.where(comp == 1, sums[1], sums[2]))

    sent = []
    for i in range(PARTS):
        v = scr[i, 0:32]
        if i > 0:
            v = v + jnp.where(p < 16, unfold(get_halo(scr.at[i - 1], halo_scr.at[i - 1]), 0), 0.0)
        sent.append(jnp.concatenate([v, scr[i, 32:64]], axis=0))
    residual = jnp.concatenate(sent, axis=1) * free
    direction = residual
    trace = jnp.zeros_like(residual)
    now = total(residual, residual)
    for step in range(CG_STEPS):
        vector = vector_of(direction)
        image = assemble(operator(jnp.concatenate([vector * first_scale, vector * second_scale], axis=0)))
        alpha = now / total(direction, image)
        trace = trace + alpha * direction
        if step + 1 < CG_STEPS:
            residual = residual - alpha * image
            fresh = total(residual, residual)
            direction = residual + (fresh / now) * direction
            now = fresh
    pieces = parts(trace)
    for i in range(PARTS):
        scr[i, 0:64] = pieces[i]
        put_halo(scr.at[i], fold(pieces[i + 1][:32], 0) if i < 3 else jnp.zeros((8, 128), F32))
    for k, ref in enumerate((o0_ref, o1_ref, o2_ref, o3_ref)):
        ref[...] = scr[lax.rem(lax.axis_index("elem") + k, PARTS), 0:64]


def recover_kernel(t0_ref, t1_ref, t2_ref, t3_ref, x_ref, rec_high, rec_low, aux_ref, o_ref, scr, t_scr, o_scr, halo_scr, sems):
    for k, ref in enumerate((t0_ref, t1_ref, t2_ref, t3_ref)):
        t_scr[lax.rem(lax.axis_index("elem") + PARTS - k, PARTS), 0:64] = ref[...]
    second = aux_ref[20:21, :]
    p = lanes(32)[0]
    row = lax.broadcasted_iota(jnp.int32, (32, 128), 0)
    vectors = []
    for q in range(4):
        v = t_scr[q, 0:32]
        h = t_scr[q, 32:64]
        right = jnp.where(p < 48, turn(v, -16), unfold(get_halo(t_scr.at[q], halo_scr.at[q]), 48))
        vectors.append(jnp.concatenate([v, right, h, jnp.where(row == 31, second, take_top(h))], axis=0))
    turned = jnp.concatenate(vectors, axis=1).T
    kind = turned[:, 127:128]
    recovered = dot3(split(jnp.concatenate([turned * (1.0 - kind), turned * kind], axis=1)), (rec_high[...], rec_low[...]))
    wave = lax.div(4 * lax.axis_index("planes") + (lax.broadcasted_iota(jnp.int32, (8, 128), 0) & 3) + 1, 2).astype(F32)
    weight = 1.0 / (2.0 + (BETA_COEF * wave) * (BETA_COEF * wave))
    for t in range(2):
        pieces = [recovered[(2 * q + el) * 64:(2 * q + el + 1) * 64, 128 * t:128 * (t + 1)] for el in range(2) for q in range(4)]
        mine = jnp.transpose(jnp.concatenate(pieces, axis=0).reshape(8, GROUPS, 128), (1, 0, 2))
        for g in range(GROUPS):
            scr[512 * t + 8 * g:512 * t + 8 * g + 8, :] = x_ref[16 * g + 8 * t:16 * g + 8 * t + 8, :] * weight + mine[g]
    lane = lax.broadcasted_iota(jnp.int32, (4, 128), 1)

    cuts = (0, 5376, 8960, PART_NODES)

    def leaving(c, part):
        cols = slice(cuts[part], cuts[part + 1])
        return pltpu.make_async_copy(o_scr.at[c, :, cols], o_ref.at[c, :, cols], sems.at[3 * c + part])

    for c in range(3):
        current = jnp.zeros((4, 128), F32)
        for e in range(2 * GROUPS):
            tile, offset = divmod(NODE * e, 128)
            rows = jnp.concatenate([scr[4 * e:4 * e + 4, :], scr[512 + 4 * e:516 + 4 * e, :]], axis=1)
            turned = pltpu.roll(rows, (offset - NODE * c) % 256, 1)
            current = jnp.where(lane >= offset, turned[:, :128], current)
            if offset + NODE >= 128:
                o_scr[c, :, 128 * tile:128 * (tile + 1)] = current
                current = turned[:, 128:]
                if 128 * (tile + 1) in cuts:
                    leaving(c, cuts.index(128 * (tile + 1)) - 1).start()
    for c in range(3):
        for part in range(3):
            leaving(c, part).wait()


VMEM = pl.BlockSpec(memory_space=pltpu.VMEM)


def shape(*dims):
    return jax.ShapeDtypeStruct(dims, F32)


ANY = pl.BlockSpec(memory_space=pl.ANY)


def half(*dims):
    return jax.ShapeDtypeStruct(dims, BF16)


def call(kernel, name, out, args, scratch=(), sems=(), far_in=False, far_out=False):
    many = isinstance(out, tuple)
    if not far_in:
        args = tuple(pltpu.with_memory_space_constraint(jnp.asarray(a), pltpu.VMEM) for a in args)
    if not far_out:
        outs = tuple(pltpu.VMEM(o.shape, o.dtype) for o in (out if many else (out,)))
        out = outs if many else outs[0]
    place = ANY if far_out else VMEM
    return pl.pallas_call(
        kernel,
        name=name,
        out_shape=out,
        in_specs=[ANY if far_in else VMEM] * len(args),
        out_specs=tuple(place for _ in out) if many else place,
        scratch_shapes=[pltpu.VMEM(dims, F32) for dims in scratch] + [pltpu.SemaphoreType.DMA((n,)) for n in sems],
    )(*args)


def exchange(value, axis, count):
    return lax.all_to_all(value.reshape(count, -1, 128), axis, split_axis=0, concat_axis=0, tiled=True)


def spread(blocks):
    moved = [lax.ppermute(blocks[k], "elem", [(s, (s + k) % PARTS) for s in range(PARTS)]) for k in range(1, PARTS)]
    return (blocks[0],) + tuple(moved)


def per_device(velocity, geometry, element_kind, element_scale, dirichlet, schur_stiffness, schur_mass, lift, recover):
    edge, node, mask_rn, mask_rr, perm, pick = selections()
    packed = call(pack_kernel, "pack", shape(1024, 128), (velocity,),
                  scratch=((3, 4, PART_NODES), (1024, 128)), sems=(len(PACK_IN), len(PACK_OUT)), far_in=True, far_out=True)
    arrived = exchange(packed, "planes", GROUPS).reshape(1024, 128)
    lift_high, lift_low, w_all, rec_high, rec_low, geo, aux = call(
        prep_kernel, "prep",
        (half(256, 256), half(256, 256), half(256, 256), half(256, 256), half(256, 256), shape(8, 256), shape(24, 128)),
        (geometry, element_kind.reshape(1, 128), element_scale.reshape(1, 128), dirichlet,
         schur_stiffness, schur_mass, lift, recover, edge, node, mask_rn, mask_rr, perm),
        scratch=((24, 128),))
    inter = call(advect_kernel, "advect", shape(1024, 128), (arrived,) + tables() + (geo,),
                 scratch=((512, 256), (512, 256), (256, 256)))
    owned = exchange(inter, "planes", GROUPS).reshape(1024, 128)
    lifted = call(lift_kernel, "lift", (shape(88, 128),) * PARTS, (owned, lift_high, lift_low, aux),
                  scratch=((512, 256), (PARTS, 88, 128)))
    traces = call(cg_kernel, "cg", (shape(64, 128),) * PARTS, spread(lifted) + (w_all, pick),
                  scratch=((PARTS, 88, 128), (PARTS, 8, 128)))
    return call(recover_kernel, "recover", shape(3, 4, PART_NODES), spread(traces) + (owned, rec_high, rec_low, aux),
                scratch=((1024, 128), (PARTS, 88, 128), (3, 4, PART_NODES), (PARTS, 8, 128)), sems=(9,), far_out=True)


def solution(mesh):
    in_specs = (
        P(None, "planes", "elem"),
        P(None, "elem"),
        P("elem"),
        P("elem"),
        P(None, None, "elem"),
        P(),
        P(),
        P(),
        P(),
    )
    out_specs = P(None, "planes", "elem")
    return jax.shard_map(per_device, mesh=mesh, in_specs=in_specs, out_specs=out_specs, check_vma=False)
```
